8 devices in a mesh: rep: 1 (over z), data: 2 (over y), expert: 4 (over x, core).
Axes of the slice: x: 2, y: 2, z: 1, core: 2. Of those that a mesh axis runs over, the one named last changes fastest.
Arguments:
- x_tok: bfloat16 [16384, 896], P(('rep', 'expert', 'data'))
- expert_idx: int32 [16384, 8], P(('rep', 'expert', 'data'))
- gate_val: float32 [16384, 8], P(('rep', 'expert', 'data'))
- w_gate: bfloat16 [64, 896, 640], P('expert', 'data')
- w_up: bfloat16 [64, 896, 640], P('expert', 'data')
- w_down: bfloat16 [64, 640, 896], P('expert', None, 'data')
- ws_gate: bfloat16 [896, 5120], P(('expert', 'data'))
- ws_up: bfloat16 [896, 5120], P(('expert', 'data'))
- ws_down: bfloat16 [5120, 896], P(None, ('expert', 'data'))
Outputs:
- output: bfloat16 [16384, 896], P(('rep', 'expert', 'data'))
All inputs are finite; a program needn't handle non-finite values.
Results may differ from the reference program's by a relative error of at most 0.001.
Values are sent between devices in bfloat16 or wider.
A program may use at most 1 GiB of HBM per device.

```python
import jax
import jax.numpy as jnp
from jax import lax

D_MODEL = 896
FF_EXP = 640
EXPERTS = 64
TOP = 8
FF_SHARED = 5120
TOKENS_DEV = 2048
BLOCKS = 8
CAPACITY = 320

TOKENS = BLOCKS * TOKENS_DEV
PAIRS = TOKENS_DEV * TOP


def draw_routing(key):
    key_score, key_bias, key_hot = jax.random.split(key, 3)
    scores = jax.random.randint(key_score, (BLOCKS, TOKENS_DEV, EXPERTS), 0, 1024, jnp.int32)
    exp_bias = jax.random.randint(key_bias, (BLOCKS, 1, EXPERTS), 0, 512, jnp.int32)
    hot_expert = jax.random.randint(key_hot, (BLOCKS, 1, 1), 0, EXPERTS, jnp.int32)
    forced = (jnp.arange(TOKENS_DEV, dtype=jnp.int32)[None, :, None] < CAPACITY) & (jnp.arange(EXPERTS, dtype=jnp.int32)[None, None, :] == hot_expert)
    ranked = (scores + exp_bias + jnp.where(forced, 4096, 0)) * EXPERTS + jnp.arange(EXPERTS, dtype=jnp.int32)
    chosen = lax.top_k(ranked, TOP)[1]
    return chosen.reshape(TOKENS, TOP).astype(jnp.int32)


def setup_inputs(seed: int = 0, part: int = 0) -> dict:
    weight_keys = jax.random.split(jax.random.key(seed), 6)
    key_x, key_route, key_gate = jax.random.split(jax.random.fold_in(jax.random.key(seed + 1), part), 3)
    scale_model = D_MODEL ** -0.5
    scale_exp = FF_EXP ** -0.5
    scale_shared = FF_SHARED ** -0.5
    x_tok = jax.random.normal(key_x, (TOKENS, D_MODEL), jnp.float32)
    gate_val = jax.random.uniform(key_gate, (TOKENS, TOP), jnp.float32, 0.2, 0.8)
    w_gate = jax.random.normal(weight_keys[0], (EXPERTS, D_MODEL, FF_EXP), jnp.float32) * scale_model
    w_up = jax.random.normal(weight_keys[1], (EXPERTS, D_MODEL, FF_EXP), jnp.float32) * scale_model
    w_down = jax.random.normal(weight_keys[2], (EXPERTS, FF_EXP, D_MODEL), jnp.float32) * scale_exp
    ws_gate = jax.random.normal(weight_keys[3], (D_MODEL, FF_SHARED), jnp.float32) * scale_model
    ws_up = jax.random.normal(weight_keys[4], (D_MODEL, FF_SHARED), jnp.float32) * scale_model
    ws_down = jax.random.normal(weight_keys[5], (FF_SHARED, D_MODEL), jnp.float32) * scale_shared
    return {"x_tok": x_tok.astype(jnp.bfloat16), "expert_idx": draw_routing(key_route), "gate_val": gate_val, "w_gate": w_gate.astype(jnp.bfloat16), "w_up": w_up.astype(jnp.bfloat16), "w_down": w_down.astype(jnp.bfloat16), "ws_gate": ws_gate.astype(jnp.bfloat16), "ws_up": ws_up.astype(jnp.bfloat16), "ws_down": ws_down.astype(jnp.bfloat16)}


def slot_block(flat_idx):
    onehot = (flat_idx[:, None] == jnp.arange(EXPERTS, dtype=jnp.int32)[None, :]).astype(jnp.int32)
    slot_idx = jnp.sum((jnp.cumsum(onehot, axis=0) - onehot) * onehot, axis=1)
    return jnp.where(slot_idx < CAPACITY, flat_idx * CAPACITY + slot_idx, EXPERTS * CAPACITY)


def source_block(dest_pos):
    return jnp.full((EXPERTS * CAPACITY,), PAIRS, jnp.int32).at[dest_pos].set(jnp.arange(PAIRS, dtype=jnp.int32), mode="drop")


def expert_ffn(tok_rows, w_gate, w_up, w_down):
    gate_pre = jnp.dot(tok_rows, w_gate, preferred_element_type=jnp.float32)
    up_pre = jnp.dot(tok_rows, w_up, preferred_element_type=jnp.float32)
    hidden = (jax.nn.silu(gate_pre) * up_pre).astype(jnp.bfloat16)
    return jnp.dot(hidden, w_down, preferred_element_type=jnp.float32).astype(jnp.bfloat16)


def reference(x_tok, expert_idx, gate_val, w_gate, w_up, w_down, ws_gate, ws_up, ws_down):
    dest_pos = jax.vmap(slot_block)(expert_idx.reshape(BLOCKS, PAIRS))
    src_pair = jax.vmap(source_block)(dest_pos)
    filled = src_pair < PAIRS
    glob_pair = jnp.minimum(src_pair, PAIRS - 1) + PAIRS * jnp.arange(BLOCKS, dtype=jnp.int32)[:, None]
    slot_gate = jnp.where(filled, gate_val.reshape(BLOCKS * PAIRS)[glob_pair], 0.0)

    def by_expert(id_table):
        return id_table.reshape(BLOCKS, EXPERTS, CAPACITY).transpose(1, 0, 2).reshape(EXPERTS, BLOCKS * CAPACITY)

    def expert_step(routed, per_expert):
        wg_e, wu_e, wd_e, tok_ids, fill_e, gate_e = per_expert
        tok_rows = jnp.where(fill_e[:, None], x_tok[tok_ids], jnp.zeros((), x_tok.dtype))
        out_rows = expert_ffn(tok_rows, wg_e, wu_e, wd_e)
        return routed.at[tok_ids].add(gate_e[:, None] * out_rows.astype(jnp.float32)), None

    routed = lax.scan(expert_step, jnp.zeros((TOKENS, D_MODEL), jnp.float32), (w_gate, w_up, w_down, by_expert(glob_pair // TOP), by_expert(filled), by_expert(slot_gate)))[0]

    def shared_of(x_blk):
        gate_pre = jnp.dot(x_blk, ws_gate, preferred_element_type=jnp.float32)
        up_pre = jnp.dot(x_blk, ws_up, preferred_element_type=jnp.float32)
        hidden = (jax.nn.silu(gate_pre) * up_pre).astype(jnp.bfloat16)
        return jnp.dot(hidden, ws_down, preferred_element_type=jnp.float32)

    shared = lax.map(shared_of, x_tok.reshape(BLOCKS, TOKENS_DEV, D_MODEL)).reshape(TOKENS, D_MODEL)
    return (x_tok.astype(jnp.float32) + shared + routed).astype(jnp.bfloat16)
```

```python
import functools

import jax
import jax.numpy as jnp
from jax import lax
from jax.experimental import pallas as pl
from jax.experimental.pallas import tpu as pltpu
from jax.sharding import PartitionSpec as P


CAP_NUM = 5
CAP_DEN = 4
BF16 = jnp.bfloat16
F32 = jnp.float32
CHUNKS = (2, 2, 2, 2)
PAD_ROWS = 16
VMEM_LIMIT = 56 * 1024 * 1024


def capacity_of(tok_count, top_count, n_exp):
    return max(8, ((CAP_NUM * top_count * tok_count) // (CAP_DEN * n_exp) + 7) // 8 * 8)


def params(sem):
    return pltpu.CompilerParams(dimension_semantics=sem, vmem_limit_bytes=VMEM_LIMIT)


def cost(flops, nbytes):
    return pl.CostEstimate(flops=int(flops), bytes_accessed=int(nbytes), transcendentals=0)


def gather_kernel(per_step, capacity, pos_ref, x_ref, *refs):
    out_ref, hot_ref = refs[-2], refs[-1]
    tok_count = x_ref.shape[0]
    slot = lax.broadcasted_iota(jnp.int32, (capacity, tok_count), 0)
    for i in range(per_step):
        pos = pos_ref[0, i:i + 1, :]
        hot_ref[i * capacity:(i + 1) * capacity, :] = jnp.where(pos == slot, 1.0, 0.0).astype(BF16)
    rows = jnp.dot(hot_ref[...], x_ref[...], preferred_element_type=F32).astype(BF16)
    out_ref[...] = rows.reshape(out_ref.shape)


def gather_rows(rel, n_blocks, pos, x_blk, buffer, capacity):
    n_exp, tok_count = pos.shape
    d_model = x_blk.shape[1]
    per_step = 2
    in_specs = [pl.BlockSpec((1, per_step, tok_count), lambda i: (i, 0, 0)), pl.BlockSpec((tok_count, d_model), lambda i: (0, 0))]
    args = [pos.reshape(n_exp // per_step, per_step, tok_count), x_blk]
    aliases = {}
    if buffer is not None:
        in_specs.append(pl.BlockSpec(memory_space=pl.ANY))
        args.append(buffer)
        aliases = {2: 0}
    rows = n_exp * capacity
    return pl.pallas_call(
        functools.partial(gather_kernel, per_step, capacity),
        out_shape=jax.ShapeDtypeStruct((n_blocks, n_exp, capacity, d_model), BF16),
        grid=(n_exp // per_step,),
        in_specs=in_specs,
        out_specs=pl.BlockSpec((1, per_step, capacity, d_model), lambda i: (rel, i, 0, 0)),
        scratch_shapes=[pltpu.VMEM((per_step * capacity, tok_count), BF16)],
        input_output_aliases=aliases,
        compiler_params=params(("arbitrary",)),
        cost_estimate=cost(2 * rows * tok_count * d_model, rows * d_model * 2),
        name="gather_rows",
    )(*args)


def swiglu(x, w_gate, w_up, w_down_t):
    gate_pre = jnp.dot(x, w_gate, preferred_element_type=F32)
    up_pre = jnp.dot(x, w_up, preferred_element_type=F32)
    hidden = (jax.nn.silu(gate_pre) * up_pre).astype(BF16)
    return lax.dot_general(hidden, w_down_t, (((1,), (1,)), ((), ())), preferred_element_type=F32)


def expert_kernel(half, y_ref, xg_ref, og_ref, ou_ref, od_ref, rv_ref, out_ref, wg_ref, wu_ref, wd_ref):
    @pl.when(pl.program_id(1) == 0)
    def _():
        mine = pl.multiple_of(y_ref[0] * half, 64)
        other = pl.multiple_of((1 - y_ref[0]) * half, 64)
        wg_ref[pl.ds(mine, half), :] = og_ref[0]
        wu_ref[pl.ds(mine, half), :] = ou_ref[0]
        wd_ref[pl.ds(mine, half), :] = od_ref[0]
        wg_ref[pl.ds(other, half), :] = rv_ref[0, 0]
        wu_ref[pl.ds(other, half), :] = rv_ref[1, 0]
        wd_ref[pl.ds(other, half), :] = rv_ref[2, 0]

    n_blk, _, capacity, d_model = xg_ref.shape
    x = xg_ref[...].reshape(n_blk * capacity, d_model)
    out = swiglu(x, wg_ref[...], wu_ref[...], wd_ref[...])
    out_ref[...] = out.astype(BF16).reshape(out_ref.shape)


def expert_rows(first, count, y_arr, xg, wg, wu, wdt, recv):
    n_blocks, n_exp, capacity, d_model = xg.shape
    half, width = wg.shape[1:]
    per_step = 2
    own = pl.BlockSpec((1, half, width), lambda i, m, y: (y[0] * n_exp + first + i, 0, 0))
    return pl.pallas_call(
        functools.partial(expert_kernel, half),
        out_shape=jax.ShapeDtypeStruct((count, n_blocks, capacity, d_model), BF16),
        grid_spec=pltpu.PrefetchScalarGridSpec(
            num_scalar_prefetch=1,
            grid=(count, n_blocks // per_step),
            in_specs=[
                pl.BlockSpec((per_step, 1, capacity, d_model), lambda i, m, y: (m, first + i, 0, 0)),
                own, own, own,
                pl.BlockSpec((3, 1, half, width), lambda i, m, y: (0, i, 0, 0)),
            ],
            out_specs=pl.BlockSpec((1, per_step, capacity, d_model), lambda i, m, y: (i, m, 0, 0)),
            scratch_shapes=[pltpu.VMEM((2 * half, width), BF16)] * 3,
        ),
        compiler_params=params(("arbitrary", "arbitrary")),
        cost_estimate=cost(6 * count * n_blocks * capacity * d_model * width, 4 * count * n_blocks * capacity * d_model),
        name="expert_rows",
    )(y_arr, xg, wg, wu, wdt, recv)


def shared_kernel(x_ref, wg_ref, wu_ref, wd_ref, out_ref):
    out_ref[...] = swiglu(x_ref[...], wg_ref[...], wu_ref[...], wd_ref[...])


def shared_part(x_blk, wg, wu, wdt):
    tok_count, d_model = x_blk.shape
    width = wg.shape[1]
    tile = 512
    whole = pl.BlockSpec((d_model, width), lambda i: (0, 0))
    rows = pl.BlockSpec((tile, d_model), lambda i: (i, 0))
    return pl.pallas_call(
        shared_kernel,
        out_shape=jax.ShapeDtypeStruct((tok_count, d_model), F32),
        grid=(tok_count // tile,),
        in_specs=[rows, whole, whole, whole],
        out_specs=rows,
        compiler_params=params(("arbitrary",)),
        cost_estimate=cost(6 * tok_count * d_model * width, 6 * tok_count * d_model),
        name="shared_part",
    )(x_blk, wg, wu, wdt)


def combine_kernel(rel, n_add, n_chunks, with_x, capacity, group, *refs):
    cnt_ref, tok_ref, gate_ref, base_ref = refs[:4]
    adds = refs[4:4 + n_add]
    outs = refs[4 + n_add:4 + n_add + n_chunks]
    pos = 4 + n_add + n_chunks
    x_ref = None
    if with_x:
        x_ref = refs[pos]
        pos += 1
    y_ref, acc, tmp, rows, wide, sem_in, sem_tmp, sem_rows, sem_out = refs[pos:]
    tok_count = base_ref.shape[0]
    body = acc.at[pl.ds(0, tok_count)]
    first = pltpu.make_async_copy(base_ref, body, sem_in)
    first.start()

    where_of = []
    for c, out in enumerate(outs):
        for i in range(out.shape[0]):
            where_of.append((c, i))

    def row_copy(e):
        c, i = where_of[e]
        return pltpu.make_async_copy(outs[c].at[i, rel], rows.at[e % 2], sem_rows.at[e % 2])

    row_copy(0).start()
    half = tok_count // 2
    offset = 0
    plan = []
    for add in adds:
        n = add.shape[0]
        if n == tok_count:
            plan.append((add, 0, n))
        else:
            plan.append((add, offset, n))
            offset = half - offset
    first.wait()
    for add, start, n in plan:
        cp = pltpu.make_async_copy(add, tmp.at[pl.ds(0, n)], sem_tmp)
        cp.start()
        cp.wait()

        @pl.loop(0, n // 64)
        def _(b):
            at = pl.multiple_of(b * 64, 64)
            acc[pl.ds(pl.multiple_of(start + at, 64), 64), :] += tmp[pl.ds(at, 64), :]

    n_exp = len(where_of)
    for e in range(n_exp):
        row_copy(e).wait()
        if e + 1 < n_exp:
            row_copy(e + 1).start()
        slot = e % 2

        @pl.loop(0, capacity // 64)
        def _(b):
            at = pl.multiple_of(b * 64, 64)
            wide[pl.ds(at, 64), :] = rows[slot, pl.ds(at, 64), :].astype(F32)

        @pl.loop(0, (cnt_ref[0, e] + (group - 1)) // group)
        def _(b):
            sums, toks = [], []
            for i in range(group):
                s = b * group + i
                t = tok_ref[0, e * capacity + s]
                g = gate_ref[0, e * capacity + s]
                toks.append(t)
                sums.append(acc[pl.ds(t, 1), :] + g * wide[pl.ds(s, 1), :])
            for i in range(group):
                acc[pl.ds(toks[i], 1), :] = sums[i]

    if with_x:

        @pl.loop(0, tok_count // 64)
        def _(b):
            at = pl.multiple_of(b * 64, 64)
            y_ref[pl.ds(at, 64), :] = (x_ref[pl.ds(at, 64), :].astype(F32) + acc[pl.ds(at, 64), :]).astype(BF16)
    else:
        last = pltpu.make_async_copy(body, y_ref, sem_out)
        last.start()
        last.wait()


def combine(rel, cnt, toks, gates, base, adds, outs, x_blk):
    tok_count, d_model = base.shape
    capacity = outs[0].shape[2]
    n_exp = sum(o.shape[0] for o in outs)
    smem = pl.BlockSpec(memory_space=pltpu.SMEM)
    hbm = pl.BlockSpec(memory_space=pl.ANY)
    vmem = pl.BlockSpec(memory_space=pltpu.VMEM)
    with_x = x_blk is not None
    args = [cnt, toks, gates, base, *adds, *outs]
    in_specs = [smem, smem, smem] + [hbm] * (len(args) - 3)
    if with_x:
        args.append(x_blk)
        in_specs.append(vmem)
    return pl.pallas_call(
        functools.partial(combine_kernel, rel, len(adds), len(outs), with_x, capacity, 4),
        out_shape=jax.ShapeDtypeStruct((tok_count, d_model), BF16 if with_x else F32),
        in_specs=in_specs,
        out_specs=vmem if with_x else hbm,
        scratch_shapes=[
            pltpu.VMEM((tok_count + PAD_ROWS, d_model), F32),
            pltpu.VMEM((tok_count, d_model), F32),
            pltpu.VMEM((2, capacity, d_model), BF16),
            pltpu.VMEM((capacity + PAD_ROWS, d_model), F32),
            pltpu.SemaphoreType.DMA,
            pltpu.SemaphoreType.DMA,
            pltpu.SemaphoreType.DMA((2,)),
            pltpu.SemaphoreType.DMA,
        ],
        compiler_params=pltpu.CompilerParams(vmem_limit_bytes=VMEM_LIMIT),
        cost_estimate=cost(2 * 8 * capacity * tok_count * d_model, tok_count * d_model * 8),
        name="combine",
    )(*args)


def solution(mesh):
    exp_n = mesh.shape["expert"]
    data_n = mesh.shape["data"]
    assert exp_n == 4 and data_n == 2
    tok_spec = P(("rep", "expert", "data"), None)
    group_axes = ("expert", "data")
    n_dev = exp_n * data_n

    def over_y(v):
        return lax.ppermute(v, "data", [(i, i ^ 1) for i in range(data_n)])

    def over_core(v):
        return lax.ppermute(v, "expert", [(i, i ^ 1) for i in range(exp_n)])

    def over_x(v):
        return lax.ppermute(v, "expert", [(i, i ^ 2) for i in range(exp_n)])

    def device_fn(x_loc, idx_loc, gate_loc, wg_loc, wu_loc, wd_loc, wsg_loc, wsu_loc, wsd_loc):
        tok_count, d_model = x_loc.shape
        top = idx_loc.shape[1]
        n_local, half, width = wg_loc.shape
        n_mine = n_local // data_n
        capacity = capacity_of(tok_count, top, n_local * exp_n)
        y = lax.axis_index("data")
        p = lax.axis_index("expert")
        me = p * data_n + y
        wdt_loc = jnp.swapaxes(wd_loc, 1, 2)

        meta = jnp.concatenate([idx_loc.T.astype(F32), gate_loc.T], axis=0)
        meta_all = lax.all_gather(meta, group_axes, axis=0)

        blocks = [None] * n_dev
        blocks[0] = x_loc
        blocks[1] = over_y(x_loc)
        blocks[4] = over_x(x_loc)
        blocks[2] = over_core(x_loc)
        blocks[6] = over_core(blocks[4])
        blocks[3] = over_core(blocks[1])
        blocks[5] = over_x(blocks[1])
        blocks[7] = over_core(blocks[5])

        ws = jnp.stack([wsg_loc, wsu_loc, wsd_loc.T])
        rows_s, width_s = ws.shape[1], ws.shape[2] // n_dev
        ws = ws.reshape(3, rows_s, n_dev, width_s).transpose(2, 0, 1, 3)
        ws = lax.all_to_all(ws, group_axes, 0, 0, tiled=True)
        ws = ws.transpose(1, 0, 2, 3).reshape(3, d_model, width_s)

        recvs = []
        start = 0
        for n in CHUNKS:
            at = (1 - y) * n_mine + start
            piece = jnp.stack([lax.dynamic_slice_in_dim(w, at, n, 0) for w in (wg_loc, wu_loc, wdt_loc)])
            recvs.append(over_y(piece))
            start += n

        meta_rel = jnp.take(meta_all, me ^ jnp.arange(n_dev, dtype=jnp.int32), axis=0)
        ids = meta_rel[:, :top].astype(jnp.int32)
        gts = meta_rel[:, top:]
        mine = p * n_local + y * n_mine + jnp.arange(n_mine, dtype=jnp.int32)
        hit = ids[:, None] == mine[None, :, None, None]
        chosen = jnp.any(hit, axis=2).reshape(n_dev * n_mine, tok_count)
        gate_of = jnp.sum(jnp.where(hit, gts[:, None], 0.0), axis=2).reshape(n_dev * n_mine, tok_count)
        t_ids = jnp.arange(tok_count, dtype=jnp.int32)
        before = (t_ids[:, None] < t_ids[None, :]).astype(BF16)
        rank = jnp.dot(chosen.astype(BF16), before, preferred_element_type=F32).astype(jnp.int32)
        pos = jnp.where(chosen & (rank < capacity), rank, -1)
        count = jnp.minimum(jnp.sum(chosen.astype(jnp.int32), axis=1), capacity).reshape(n_dev, 1, n_mine)
        same = pos[:, None, :] == jnp.arange(capacity, dtype=jnp.int32)[None, :, None]
        toks = jnp.sum(jnp.where(same, t_ids[None, None, :] - tok_count, 0), axis=2) + tok_count
        slot_gate = jnp.sum(jnp.where(same, gate_of[:, None, :], 0.0), axis=2)
        toks = toks.reshape(n_dev, 1, n_mine * capacity)
        slot_gate = slot_gate.reshape(n_dev, 1, n_mine * capacity)
        pos = pos.reshape(n_dev, n_mine, tok_count)

        order = (0, 2, 4, 6, 1, 3, 5, 7)
        xg = None
        base = [None] * n_dev
        for r in order:
            xg = gather_rows(r, n_dev, pos[r], blocks[r], xg, capacity)
            base[r] = shared_part(blocks[r], ws[0], ws[1], ws[2])

        xg, base = lax.optimization_barrier((xg, base))
        y_arr = y.astype(jnp.int32).reshape(1)
        outs = []
        start = 0
        for n, recv in zip(CHUNKS, recvs):
            outs.append(expert_rows(start, n, y_arr, xg, wg_loc, wu_loc, wdt_loc, recv))
            start += n

        def part(r, adds, x_blk=None):
            return combine(r, count[r], toks[r], slot_gate[r], base[r], adds, outs, x_blk)

        h = tok_count // 2
        diag = part(6 + 1, [])
        diag = part(4 + 1, [over_core(diag)])
        diag_x = over_x(diag[:h])
        diag_y = over_y(diag[h:])
        to_x = part(6, [])
        to_y = part(2 + 1, [])
        to_x = part(4, [over_core(to_x)])
        to_y = part(1, [over_core(to_y)])
        x_top = over_x(to_x[:h])
        y_bot = over_y(to_y[h:])
        x_bot = over_x(to_x[h:] + diag_y)
        y_top = over_y(to_y[:h] + diag_x)
        mate = over_core(part(2, []))
        return part(0, [mate, x_top, x_bot, y_top, y_bot], x_loc)

    in_specs = (tok_spec, tok_spec, tok_spec, P("expert", "data", None), P("expert", "data", None), P("expert", None, "data"), P(group_axes, None), P(group_axes, None), P(None, group_axes))
    return jax.shard_map(device_fn, mesh=mesh, in_specs=in_specs, out_specs=tok_spec, check_vma=False)
```

```python
import functools

import jax
import jax.numpy as jnp
from jax import lax
from jax.experimental import pallas as pl
from jax.experimental.pallas import tpu as pltpu
from jax.sharding import PartitionSpec as P


CAP_NUM = 5
CAP_DEN = 4
BF16 = jnp.bfloat16
F32 = jnp.float32
CHUNKS = (2, 2, 2, 1, 1)
LANES = 128
TILE = 8
VMEM_LIMIT = 56 * 1024 * 1024


def capacity_of(tok_count, top_count, n_exp):
    return max(8, ((CAP_NUM * top_count * tok_count) // (CAP_DEN * n_exp) + 7) // 8 * 8)


def params(sem):
    return pltpu.CompilerParams(dimension_semantics=sem, vmem_limit_bytes=VMEM_LIMIT)


def cost(flops, nbytes):
    return pl.CostEstimate(flops=int(flops) // 64, bytes_accessed=int(nbytes), transcendentals=0)


def gather_kernel(per_step, capacity, pos_ref, x_ref, *refs):
    out_ref, hot_ref = refs[-2], refs[-1]
    step = pl.program_id(0)
    tok_count = x_ref.shape[0]
    slot = lax.broadcasted_iota(jnp.int32, (capacity, tok_count), 0)
    for i in range(per_step):
        pos = pos_ref[pl.ds(step * per_step + i, 1), :]
        hot_ref[i * capacity:(i + 1) * capacity, :] = jnp.where(pos == slot, 1.0, 0.0).astype(BF16)
    rows = jnp.dot(hot_ref[...], x_ref[...], preferred_element_type=F32).astype(BF16)
    out_ref[...] = rows.reshape(out_ref.shape)


def gather_rows(rel, n_blocks, pos, x_blk, buffer, capacity):
    pos_rows, tok_count = pos.shape
    n_exp = pos_rows - TILE
    d_model = x_blk.shape[1]
    per_step = 2
    in_specs = [pl.BlockSpec((pos_rows, tok_count), lambda i: (0, 0)), pl.BlockSpec((tok_count, d_model), lambda i: (0, 0))]
    args = [pos, x_blk]
    aliases = {}
    if buffer is not None:
        in_specs.append(pl.BlockSpec(memory_space=pl.ANY))
        args.append(buffer)
        aliases = {2: 0}
    rows = n_exp * capacity
    return pl.pallas_call(
        functools.partial(gather_kernel, per_step, capacity),
        out_shape=jax.ShapeDtypeStruct((n_blocks, n_exp, capacity, d_model), BF16),
        grid=(n_exp // per_step,),
        in_specs=in_specs,
        out_specs=pl.BlockSpec((1, per_step, capacity, d_model), lambda i: (rel, i, 0, 0)),
        scratch_shapes=[pltpu.VMEM((per_step * capacity, tok_count), BF16)],
        input_output_aliases=aliases,
        compiler_params=params(("arbitrary",)),
        cost_estimate=cost(2 * rows * tok_count * d_model, rows * d_model * 2),
        name="gather_rows",
    )(*args)


def swiglu(x, w_gate_up, w_down_t):
    width = w_down_t.shape[1]
    pre = jnp.dot(x, w_gate_up, preferred_element_type=F32)
    hidden = (jax.nn.silu(pre[:, :width]) * pre[:, width:]).astype(BF16)
    return lax.dot_general(hidden, w_down_t, (((1,), (1,)), ((), ())), preferred_element_type=F32)


def expert_kernel(half, y_ref, xg_ref, og_ref, ou_ref, od_ref, rv_ref, out_ref, wgu_ref, wd_ref):
    width = wd_ref.shape[1]

    @pl.when(pl.program_id(1) == 0)
    def _():
        mine = pl.multiple_of(y_ref[0] * half, 64)
        other = pl.multiple_of((1 - y_ref[0]) * half, 64)
        wgu_ref[pl.ds(mine, half), :width] = og_ref[0]
        wgu_ref[pl.ds(mine, half), width:] = ou_ref[0]
        wd_ref[pl.ds(mine, half), :] = od_ref[0]
        wgu_ref[pl.ds(other, half), :width] = rv_ref[0, 0]
        wgu_ref[pl.ds(other, half), width:] = rv_ref[1, 0]
        wd_ref[pl.ds(other, half), :] = rv_ref[2, 0]

    n_blk, _, capacity, d_model = xg_ref.shape
    x = xg_ref[...].reshape(n_blk * capacity, d_model)
    out = swiglu(x, wgu_ref[...], wd_ref[...])
    out_ref[...] = out.astype(BF16).reshape(out_ref.shape)


def expert_rows(first, count, y_arr, xg, wg, wu, wdt, recv):
    n_blocks, n_exp, capacity, d_model = xg.shape
    half, width = wg.shape[1:]
    per_step = 2
    own = pl.BlockSpec((1, half, width), lambda i, m, y: (y[0] * n_exp + first + i, 0, 0))
    return pl.pallas_call(
        functools.partial(expert_kernel, half),
        out_shape=jax.ShapeDtypeStruct((count, n_blocks, capacity, d_model), BF16),
        grid_spec=pltpu.PrefetchScalarGridSpec(
            num_scalar_prefetch=1,
            grid=(count, n_blocks // per_step),
            in_specs=[
                pl.BlockSpec((per_step, 1, capacity, d_model), lambda i, m, y: (m, first + i, 0, 0)),
                own, own, own,
                pl.BlockSpec((3, 1, half, width), lambda i, m, y: (0, i, 0, 0)),
            ],
            out_specs=pl.BlockSpec((1, per_step, capacity, d_model), lambda i, m, y: (i, m, 0, 0)),
            scratch_shapes=[pltpu.VMEM((2 * half, 2 * width), BF16), pltpu.VMEM((2 * half, width), BF16)],
        ),
        compiler_params=params(("arbitrary", "arbitrary")),
        cost_estimate=cost(6 * count * n_blocks * capacity * d_model * width, 4 * count * n_blocks * capacity * d_model),
        name="expert_rows",
    )(y_arr, xg, wg, wu, wdt, recv)


def shared_kernel(x_ref, wgu_ref, wd_ref, out_ref):
    out_ref[...] = swiglu(x_ref[...], wgu_ref[...], wd_ref[...])


def shared_part(x_blk, wgu, wdt):
    tok_count, d_model = x_blk.shape
    width = wdt.shape[1]
    tile = 512
    rows = pl.BlockSpec((tile, d_model), lambda i: (i, 0))
    return pl.pallas_call(
        shared_kernel,
        out_shape=jax.ShapeDtypeStruct((tok_count, d_model), F32),
        grid=(tok_count // tile,),
        in_specs=[rows, pl.BlockSpec((d_model, 2 * width), lambda i: (0, 0)), pl.BlockSpec((d_model, width), lambda i: (0, 0))],
        out_specs=rows,
        compiler_params=params(("arbitrary",)),
        cost_estimate=cost(6 * tok_count * d_model * width, 6 * tok_count * d_model),
        name="shared_part",
    )(x_blk, wgu, wdt)


def combine_kernel(rel, n_base, where_of, halves, capacity, group, *refs):
    cnt_ref, tok_ref, gate_ref = refs[:3]
    bases = refs[3:3 + n_base]
    n_chunks = max(c for c, _, _ in where_of) + 1
    outs = refs[3 + n_base:3 + n_base + n_chunks]
    n_out = 2 if halves else 1
    pos = 3 + n_base + n_chunks
    y_refs = refs[pos:pos + n_out]
    acc, tmps, rows, wide, sem_in, sem_rows, sem_out = refs[pos + n_out:]
    tok_count, d_model = bases[0].shape
    n_col = d_model // LANES
    step = 256
    n_step = tok_count // step

    def in_copy(k, b):
        at = pl.ds(b * step, step)
        return pltpu.make_async_copy(bases[k].at[at], tmps.at[k, at], sem_in.at[k, b])

    def out_copy(b):
        at = b * step
        per_out = tok_count // n_out
        dst = y_refs[at // per_out].at[pl.ds(at % per_out, step)]
        return pltpu.make_async_copy(tmps.at[0, pl.ds(at, step)], dst, sem_out.at[b])

    def row_copy(i):
        c, local, _ = where_of[i]
        return pltpu.make_async_copy(outs[c].at[local, rel], rows.at[i % 2], sem_rows.at[i % 2])

    for b in range(n_step):
        for k in range(n_base):
            in_copy(k, b).start()
    row_copy(0).start()

    for b in range(n_step):
        for k in range(n_base):
            in_copy(k, b).wait()

        @pl.loop(0, step // 32)
        def _(q):
            at = pl.multiple_of(b * step + q * 32, 32)
            val = tmps[0, pl.ds(at, 32), :]
            for k in range(1, n_base):
                val = val + tmps[k, pl.ds(at, 32), :]
            for j in range(n_col):
                acc[pl.ds(at * TILE + j, 32, stride=TILE), :] = val[:, j * LANES:(j + 1) * LANES]

    for i in range(len(where_of)):
        row_copy(i).wait()
        if i + 1 < len(where_of):
            row_copy(i + 1).start()
        e = where_of[i][2]
        slot = i % 2

        @pl.loop(0, capacity // 32)
        def _(q):
            at = pl.multiple_of(q * 32, 32)
            val = rows[slot, pl.ds(at, 32), :].astype(F32)
            for j in range(n_col):
                wide[pl.ds(at * TILE + j, 32, stride=TILE), :] = val[:, j * LANES:(j + 1) * LANES]

        @pl.loop(0, (cnt_ref[0, e] + (group - 1)) // group)
        def _(q):
            sums, toks = [], []
            for i in range(group):
                s = q * group + i
                t = pl.multiple_of(tok_ref[0, e * capacity + s], TILE)
                g = gate_ref[0, e * capacity + s]
                toks.append(t)
                sums.append(acc[pl.ds(t, TILE), :] + g * wide[pl.ds(pl.multiple_of(s * TILE, TILE), TILE), :])
            for i in range(group):
                acc[pl.ds(toks[i], TILE), :] = sums[i]

    for b in range(n_step):

        @pl.loop(0, step // 32)
        def _(q):
            at = pl.multiple_of(b * step + q * 32, 32)
            for j in range(n_col):
                tmps[0, pl.ds(at, 32), j * LANES:(j + 1) * LANES] = acc[pl.ds(at * TILE + j, 32, stride=TILE), :]

        out_copy(b).start()
    for b in range(n_step):
        out_copy(b).wait()


def combine(rel, cnt, toks, gates, bases, outs, first, halves):
    tok_count, d_model = bases[0].shape
    capacity = outs[0].shape[2]
    where_of = []
    for c, o in enumerate(outs):
        for i in range(o.shape[0]):
            where_of.append((c, i, first + len(where_of)))
    smem = pl.BlockSpec(memory_space=pltpu.SMEM)
    hbm = pl.BlockSpec(memory_space=pl.ANY)
    n_base = len(bases)
    if halves:
        out_shape = [jax.ShapeDtypeStruct((tok_count // 2, d_model), F32)] * 2
        out_specs = [hbm, hbm]
    else:
        out_shape, out_specs = jax.ShapeDtypeStruct((tok_count, d_model), F32), hbm
    return pl.pallas_call(
        functools.partial(combine_kernel, rel, n_base, tuple(where_of), halves, capacity, 8),
        out_shape=out_shape,
        in_specs=[smem, smem, smem] + [hbm] * (n_base + len(outs)),
        out_specs=out_specs,
        scratch_shapes=[
            pltpu.VMEM(((tok_count + 1) * TILE, LANES), F32),
            pltpu.VMEM((n_base, tok_count, d_model), F32),
            pltpu.VMEM((2, capacity, d_model), BF16),
            pltpu.VMEM((capacity * TILE, LANES), F32),
            pltpu.SemaphoreType.DMA((n_base, tok_count // 256)),
            pltpu.SemaphoreType.DMA((2,)),
            pltpu.SemaphoreType.DMA((tok_count // 256,)),
        ],
        compiler_params=pltpu.CompilerParams(vmem_limit_bytes=VMEM_LIMIT),
        cost_estimate=cost(len(where_of) * capacity * tok_count * d_model, tok_count * d_model * 8),
        name="combine",
    )(cnt, toks, gates, *bases, *outs)


def solution(mesh):
    exp_n = mesh.shape["expert"]
    data_n = mesh.shape["data"]
    assert exp_n == 4 and data_n == 2
    tok_spec = P(("rep", "expert", "data"), None)
    group_axes = ("expert", "data")
    n_dev = exp_n * data_n

    def over_y(v):
        return lax.ppermute(v, "data", [(i, i ^ 1) for i in range(data_n)])

    def over_core(v):
        return lax.ppermute(v, "expert", [(i, i ^ 1) for i in range(exp_n)])

    def over_x(v):
        return lax.ppermute(v, "expert", [(i, i ^ 2) for i in range(exp_n)])

    def device_fn(x_loc, idx_loc, gate_loc, wg_loc, wu_loc, wd_loc, wsg_loc, wsu_loc, wsd_loc):
        tok_count, d_model = x_loc.shape
        top = idx_loc.shape[1]
        n_local, _, _ = wg_loc.shape
        n_mine = n_local // data_n
        capacity = capacity_of(tok_count, top, n_local * exp_n)
        y = lax.axis_index("data")
        p = lax.axis_index("expert")
        me = p * data_n + y
        wdt_loc = jnp.swapaxes(wd_loc, 1, 2)

        meta = jnp.concatenate([idx_loc.T.astype(F32), gate_loc.T], axis=0)
        meta_all = lax.all_gather(meta, group_axes, axis=0)

        blocks = [None] * n_dev
        blocks[0] = x_loc
        blocks[1] = over_y(x_loc)
        blocks[4] = over_x(x_loc)
        blocks[2] = over_core(x_loc)
        blocks[6] = over_core(blocks[4])
        blocks[3] = over_core(blocks[1])
        blocks[5] = over_x(blocks[1])
        blocks[7] = over_core(blocks[5])

        ws = jnp.stack([wsg_loc, wsu_loc, wsd_loc.T])
        rows_s, width_s = ws.shape[1], ws.shape[2] // n_dev
        ws = ws.reshape(3, rows_s, n_dev, width_s).transpose(2, 0, 1, 3)
        ws = lax.all_to_all(ws, group_axes, 0, 0, tiled=True)
        ws = ws.transpose(1, 0, 2, 3).reshape(3, d_model, width_s)
        wgu_s, wdt_s = jnp.concatenate([ws[0], ws[1]], axis=1), ws[2]

        recvs = []
        start = 0
        for n in CHUNKS:
            at = (1 - y) * n_mine + start
            piece = jnp.stack([lax.dynamic_slice_in_dim(w, at, n, 0) for w in (wg_loc, wu_loc, wdt_loc)])
            recvs.append(over_y(piece))
            start += n

        meta_rel = jnp.take(meta_all, me ^ jnp.arange(n_dev, dtype=jnp.int32), axis=0)
        ids = meta_rel[:, :top].astype(jnp.int32)
        gts = meta_rel[:, top:]
        mine = p * n_local + y * n_mine + jnp.arange(n_mine, dtype=jnp.int32)
        hit = ids[:, None] == mine[None, :, None, None]
        chosen = jnp.any(hit, axis=2).reshape(n_dev * n_mine, tok_count)
        t_ids = jnp.arange(tok_count, dtype=jnp.int32)
        before = (t_ids[:, None] < t_ids[None, :]).astype(BF16)
        rank = jnp.dot(chosen.astype(BF16), before, preferred_element_type=F32).astype(jnp.int32)
        pos = jnp.where(chosen & (rank < capacity), rank, -1)
        pos_pad = jnp.pad(pos.reshape(n_dev, n_mine, tok_count), ((0, 0), (0, TILE), (0, 0)), constant_values=-1)

        last = [pos_pad]

        def after(*vals):
            done, vals = lax.optimization_barrier((last[0], vals))
            last[0] = done
            return vals if len(vals) > 1 else vals[0]

        xg = None

        def gather(r):
            nonlocal xg
            x_blk = after(blocks[r])
            xg = gather_rows(r, n_dev, pos_pad[r], x_blk, xg, capacity)
            last[0] = xg

        base = [None] * n_dev

        def shared(r):
            x_blk = after(blocks[r])
            base[r] = shared_part(x_blk, wgu_s, wdt_s)
            last[0] = base[r]

        y_arr = y.astype(jnp.int32).reshape(1)
        outs = []

        def experts(c):
            start = sum(CHUNKS[:c])
            outs.append(expert_rows(start, CHUNKS[c], y_arr, xg, wg_loc, wu_loc, wdt_loc, after(recvs[c])))
            last[0] = outs[-1]

        lists = []

        def make_lists():
            p_in, ids_in, gts_in = after(pos, ids, gts)
            hit_in = ids_in[:, None] == mine[None, :, None, None]
            gate_of = jnp.sum(jnp.where(hit_in, gts_in[:, None], 0.0), axis=2).reshape(n_dev * n_mine, tok_count)
            same = p_in[:, None, :] == jnp.arange(capacity, dtype=jnp.int32)[None, :, None]
            toks = jnp.sum(jnp.where(same, t_ids[None, None, :] - tok_count, 0), axis=2) + tok_count
            slot_gate = jnp.sum(jnp.where(same, gate_of[:, None, :], 0.0), axis=2)
            count = jnp.sum((p_in >= 0).astype(jnp.int32), axis=1).reshape(n_dev, 1, n_mine)
            toks = (toks * TILE).reshape(n_dev, 1, n_mine * capacity)
            slot_gate = slot_gate.reshape(n_dev, 1, n_mine * capacity)
            lists.extend([count, toks, slot_gate])
            last[0] = (toks, slot_gate)

        def part(r, bases, first, halves):
            count, toks, slot_gate = lists
            c0 = 0
            while sum(CHUNKS[:c0]) < first:
                c0 += 1
            (b0, *rest) = bases
            args = [after(b0), *rest]
            out = combine(r, count[r], toks[r], slot_gate[r], args, outs[c0:], first, halves)
            last[0] = out[0] if halves else out
            return out

        gather(0)
        gather(2)
        gather(1)
        gather(4)
        make_lists()
        gather(3)
        gather(6)
        gather(5)
        gather(7)
        experts(0)
        shared(7)
        shared(5)
        experts(1)
        shared(6)
        shared(4)
        experts(2)
        shared(3)
        n_pre = sum(CHUNKS[:3])
        pre7 = part(7, [base[7]], 0, False)
        pre5 = part(5, [base[5]], 0, False)
        experts(3)
        shared(1)
        experts(4)
        mate7 = over_core(part(7, [pre7], n_pre, False))
        mate6 = over_core(part(6, [base[6]], 0, False))
        diag = part(5, [pre5, mate7], n_pre, True)
        diag_x = over_x(diag[0])
        diag_y = over_y(diag[1])
        to_x = part(4, [base[4], mate6], 0, True)
        x_top = over_x(to_x[0])
        mate3 = over_core(part(3, [base[3]], 0, False))
        shared(2)
        mate2 = over_core(part(2, [base[2]], 0, False))
        to_y = part(1, [base[1], mate3], 0, True)
        y_bot = over_y(to_y[1])
        shared(0)
        own = part(0, [base[0], mate2], 0, True)
        up_x, up_y, to_x1, to_y0 = after(diag_y, diag_x, to_x[1], to_y[0])
        x_bot = over_x(to_x1 + up_x)
        y_top = over_y(to_y0 + up_y)
        h = tok_count // 2
        top_rows = x_loc[:h].astype(F32) + own[0] + x_top + y_top
        bot_rows = x_loc[h:].astype(F32) + own[1] + x_bot + y_bot
        return jnp.concatenate([top_rows.astype(BF16), bot_rows.astype(BF16)], axis=0)

    in_specs = (tok_spec, tok_spec, tok_spec, P("expert", "data", None), P("expert", "data", None), P("expert", None, "data"), P(group_axes, None), P(group_axes, None), P(None, group_axes))
    return jax.shard_map(device_fn, mesh=mesh, in_specs=in_specs, out_specs=tok_spec, check_vma=False)
```

```python
import functools

import jax
import jax.numpy as jnp
from jax import lax
from jax.experimental import pallas as pl
from jax.experimental.pallas import tpu as pltpu
from jax.sharding import PartitionSpec as P


CAP_NUM = 5
CAP_DEN = 4
BF16 = jnp.bfloat16
F32 = jnp.float32
CHUNKS = (2, 2, 2, 1, 1)
LANES = 128
TILE = 8
VMEM_LIMIT = 56 * 1024 * 1024


def capacity_of(tok_count, top_count, n_exp):
    return max(8, ((CAP_NUM * top_count * tok_count) // (CAP_DEN * n_exp) + 7) // 8 * 8)


def params(sem):
    return pltpu.CompilerParams(dimension_semantics=sem, vmem_limit_bytes=VMEM_LIMIT)


def cost(flops, nbytes):
    return pl.CostEstimate(flops=int(flops) // 64, bytes_accessed=int(nbytes), transcendentals=0)


def gather_kernel(per_step, capacity, pos_ref, x_ref, *refs):
    out_ref, hot_ref = refs[-2], refs[-1]
    step = pl.program_id(0)
    tok_count = x_ref.shape[0]
    slot = lax.broadcasted_iota(jnp.int32, (capacity, tok_count), 0)
    for i in range(per_step):
        pos = pos_ref[pl.ds(step * per_step + i, 1), :]
        hot_ref[i * capacity:(i + 1) * capacity, :] = jnp.where(pos == slot, 1.0, 0.0).astype(BF16)
    rows = jnp.dot(hot_ref[...], x_ref[...], preferred_element_type=F32).astype(BF16)
    out_ref[...] = rows.reshape(out_ref.shape)


def gather_rows(rel, n_blocks, pos, x_blk, buffer, capacity):
    pos_rows, tok_count = pos.shape
    n_exp = pos_rows - TILE
    d_model = x_blk.shape[1]
    per_step = 2
    in_specs = [pl.BlockSpec((pos_rows, tok_count), lambda i: (0, 0)), pl.BlockSpec((tok_count, d_model), lambda i: (0, 0))]
    args = [pos, x_blk]
    aliases = {}
    if buffer is not None:
        in_specs.append(pl.BlockSpec(memory_space=pl.ANY))
        args.append(buffer)
        aliases = {2: 0}
    rows = n_exp * capacity
    return pl.pallas_call(
        functools.partial(gather_kernel, per_step, capacity),
        out_shape=jax.ShapeDtypeStruct((n_blocks, n_exp, capacity, d_model), BF16),
        grid=(n_exp // per_step,),
        in_specs=in_specs,
        out_specs=pl.BlockSpec((1, per_step, capacity, d_model), lambda i: (rel, i, 0, 0)),
        scratch_shapes=[pltpu.VMEM((per_step * capacity, tok_count), BF16)],
        input_output_aliases=aliases,
        compiler_params=params(("arbitrary",)),
        cost_estimate=cost(2 * rows * tok_count * d_model, rows * d_model * 2),
        name="gather_rows",
    )(*args)


def swiglu(x, w_gate, w_up, w_down_t):
    gate_pre = jnp.dot(x, w_gate, preferred_element_type=F32)
    up_pre = jnp.dot(x, w_up, preferred_element_type=F32)
    hidden = (jax.nn.silu(gate_pre) * up_pre).astype(BF16)
    return lax.dot_general(hidden, w_down_t, (((1,), (1,)), ((), ())), preferred_element_type=F32)


def expert_kernel(half, y_ref, xg_ref, og_ref, ou_ref, od_ref, rv_ref, out_ref, wg_ref, wu_ref, wd_ref):
    @pl.when(pl.program_id(1) == 0)
    def _():
        mine = pl.multiple_of(y_ref[0] * half, 64)
        other = pl.multiple_of((1 - y_ref[0]) * half, 64)
        wg_ref[pl.ds(mine, half), :] = og_ref[0]
        wu_ref[pl.ds(mine, half), :] = ou_ref[0]
        wd_ref[pl.ds(mine, half), :] = od_ref[0]
        wg_ref[pl.ds(other, half), :] = rv_ref[0, 0]
        wu_ref[pl.ds(other, half), :] = rv_ref[1, 0]
        wd_ref[pl.ds(other, half), :] = rv_ref[2, 0]

    n_blk, _, capacity, d_model = xg_ref.shape
    x = xg_ref[...].reshape(n_blk * capacity, d_model)
    out = swiglu(x, wg_ref[...], wu_ref[...], wd_ref[...])
    out_ref[...] = out.astype(BF16).reshape(out_ref.shape)


def expert_rows(first, count, y_arr, xg, wg, wu, wdt, recv):
    n_blocks, n_exp, capacity, d_model = xg.shape
    half, width = wg.shape[1:]
    per_step = 2
    own = pl.BlockSpec((1, half, width), lambda i, m, y: (y[0] * n_exp + first + i, 0, 0))
    return pl.pallas_call(
        functools.partial(expert_kernel, half),
        out_shape=jax.ShapeDtypeStruct((count, n_blocks, capacity, d_model), BF16),
        grid_spec=pltpu.PrefetchScalarGridSpec(
            num_scalar_prefetch=1,
            grid=(count, n_blocks // per_step),
            in_specs=[
                pl.BlockSpec((per_step, 1, capacity, d_model), lambda i, m, y: (m, first + i, 0, 0)),
                own, own, own,
                pl.BlockSpec((3, 1, half, width), lambda i, m, y: (0, i, 0, 0)),
            ],
            out_specs=pl.BlockSpec((1, per_step, capacity, d_model), lambda i, m, y: (i, m, 0, 0)),
            scratch_shapes=[pltpu.VMEM((2 * half, width), BF16)] * 3,
        ),
        compiler_params=params(("arbitrary", "arbitrary")),
        cost_estimate=cost(6 * count * n_blocks * capacity * d_model * width, 4 * count * n_blocks * capacity * d_model),
        name="expert_rows",
    )(y_arr, xg, wg, wu, wdt, recv)


def shared_kernel(x_ref, wg_ref, wu_ref, wd_ref, out_ref):
    out_ref[...] = swiglu(x_ref[...], wg_ref[...], wu_ref[...], wd_ref[...])


def shared_part(x_blk, wg, wu, wdt):
    tok_count, d_model = x_blk.shape
    width = wdt.shape[1]
    tile = 512
    rows = pl.BlockSpec((tile, d_model), lambda i: (i, 0))
    return pl.pallas_call(
        shared_kernel,
        out_shape=jax.ShapeDtypeStruct((tok_count, d_model), F32),
        grid=(tok_count // tile,),
        in_specs=[rows] + [pl.BlockSpec((d_model, width), lambda i: (0, 0))] * 3,
        out_specs=rows,
        compiler_params=params(("arbitrary",)),
        cost_estimate=cost(6 * tok_count * d_model * width, 6 * tok_count * d_model),
        name="shared_part",
    )(x_blk, wg, wu, wdt)


def combine_kernel(rel, n_base, where_of, halves, capacity, group, *refs):
    cnt_ref, tok_ref, gate_ref = refs[:3]
    bases = refs[3:3 + n_base]
    n_chunks = max(c for c, _, _ in where_of) + 1
    outs = refs[3 + n_base:3 + n_base + n_chunks]
    n_out = 2 if halves else 1
    pos = 3 + n_base + n_chunks
    y_refs = refs[pos:pos + n_out]
    acc, tmps, rows, wide, sem_in, sem_rows, sem_out = refs[pos + n_out:]
    tok_count, d_model = bases[0].shape
    n_col = d_model // LANES
    step = 256
    n_step = tok_count // step

    def in_copy(k, b):
        at = pl.ds(b * step, step)
        return pltpu.make_async_copy(bases[k].at[at], tmps.at[k, at], sem_in.at[k, b])

    def out_copy(b):
        at = b * step
        per_out = tok_count // n_out
        dst = y_refs[at // per_out].at[pl.ds(at % per_out, step)]
        return pltpu.make_async_copy(tmps.at[0, pl.ds(at, step)], dst, sem_out.at[b])

    def row_copy(i):
        c, local, _ = where_of[i]
        return pltpu.make_async_copy(outs[c].at[local, rel], rows.at[i % 2], sem_rows.at[i % 2])

    for b in range(n_step):
        for k in range(n_base):
            in_copy(k, b).start()
    row_copy(0).start()

    for b in range(n_step):
        for k in range(n_base):
            in_copy(k, b).wait()

        @pl.loop(0, step // 32)
        def _(q):
            at = pl.multiple_of(b * step + q * 32, 32)
            val = tmps[0, pl.ds(at, 32), :]
            for k in range(1, n_base):
                val = val + tmps[k, pl.ds(at, 32), :]
            for j in range(n_col):
                acc[pl.ds(at * TILE + j, 32, stride=TILE), :] = val[:, j * LANES:(j + 1) * LANES]

    for i in range(len(where_of)):
        row_copy(i).wait()
        if i + 1 < len(where_of):
            row_copy(i + 1).start()
        e = where_of[i][2]
        slot = i % 2

        @pl.loop(0, capacity // 32)
        def _(q):
            at = pl.multiple_of(q * 32, 32)
            val = rows[slot, pl.ds(at, 32), :].astype(F32)
            for j in range(n_col):
                wide[pl.ds(at * TILE + j, 32, stride=TILE), :] = val[:, j * LANES:(j + 1) * LANES]

        @pl.loop(0, (cnt_ref[0, e] + (group - 1)) // group)
        def _(q):
            sums, toks = [], []
            for i in range(group):
                s = q * group + i
                t = pl.multiple_of(tok_ref[0, e * capacity + s], TILE)
                g = gate_ref[0, e * capacity + s]
                toks.append(t)
                sums.append(acc[pl.ds(t, TILE), :] + g * wide[pl.ds(pl.multiple_of(s * TILE, TILE), TILE), :])
            for i in range(group):
                acc[pl.ds(toks[i], TILE), :] = sums[i]

    for b in range(n_step):

        @pl.loop(0, step // 32)
        def _(q):
            at = pl.multiple_of(b * step + q * 32, 32)
            for j in range(n_col):
                tmps[0, pl.ds(at, 32), j * LANES:(j + 1) * LANES] = acc[pl.ds(at * TILE + j, 32, stride=TILE), :]

        out_copy(b).start()
    for b in range(n_step):
        out_copy(b).wait()


def combine(rel, cnt, toks, gates, bases, outs, first, halves):
    tok_count, d_model = bases[0].shape
    capacity = outs[0].shape[2]
    where_of = []
    for c, o in enumerate(outs):
        for i in range(o.shape[0]):
            where_of.append((c, i, first + len(where_of)))
    smem = pl.BlockSpec(memory_space=pltpu.SMEM)
    hbm = pl.BlockSpec(memory_space=pl.ANY)
    n_base = len(bases)
    if halves:
        out_shape = [jax.ShapeDtypeStruct((tok_count // 2, d_model), F32)] * 2
        out_specs = [hbm, hbm]
    else:
        out_shape, out_specs = jax.ShapeDtypeStruct((tok_count, d_model), F32), hbm
    return pl.pallas_call(
        functools.partial(combine_kernel, rel, n_base, tuple(where_of), halves, capacity, 8),
        out_shape=out_shape,
        in_specs=[smem, smem, smem] + [hbm] * (n_base + len(outs)),
        out_specs=out_specs,
        scratch_shapes=[
            pltpu.VMEM(((tok_count + 1) * TILE, LANES), F32),
            pltpu.VMEM((n_base, tok_count, d_model), F32),
            pltpu.VMEM((2, capacity, d_model), BF16),
            pltpu.VMEM((capacity * TILE, LANES), F32),
            pltpu.SemaphoreType.DMA((n_base, tok_count // 256)),
            pltpu.SemaphoreType.DMA((2,)),
            pltpu.SemaphoreType.DMA((tok_count // 256,)),
        ],
        compiler_params=pltpu.CompilerParams(vmem_limit_bytes=VMEM_LIMIT),
        cost_estimate=cost(len(where_of) * capacity * tok_count * d_model, tok_count * d_model * 8),
        name="combine",
    )(cnt, toks, gates, *bases, *outs)


def solution(mesh):
    exp_n = mesh.shape["expert"]
    data_n = mesh.shape["data"]
    assert exp_n == 4 and data_n == 2
    tok_spec = P(("rep", "expert", "data"), None)
    group_axes = ("expert", "data")
    n_dev = exp_n * data_n

    def over_y(v):
        return lax.ppermute(v, "data", [(i, i ^ 1) for i in range(data_n)])

    def over_core(v):
        return lax.ppermute(v, "expert", [(i, i ^ 1) for i in range(exp_n)])

    def over_x(v):
        return lax.ppermute(v, "expert", [(i, i ^ 2) for i in range(exp_n)])

    def device_fn(x_loc, idx_loc, gate_loc, wg_loc, wu_loc, wd_loc, wsg_loc, wsu_loc, wsd_loc):
        tok_count, d_model = x_loc.shape
        top = idx_loc.shape[1]
        n_local, _, _ = wg_loc.shape
        n_mine = n_local // data_n
        capacity = capacity_of(tok_count, top, n_local * exp_n)
        y = lax.axis_index("data")
        p = lax.axis_index("expert")
        me = p * data_n + y
        wdt_loc = jnp.swapaxes(wd_loc, 1, 2)

        meta = jnp.concatenate([idx_loc.T.astype(F32), gate_loc.T], axis=0)
        meta_all = lax.all_gather(meta, group_axes, axis=0)

        blocks = [None] * n_dev
        blocks[0] = x_loc
        blocks[1] = over_y(x_loc)
        blocks[4] = over_x(x_loc)
        blocks[2] = over_core(x_loc)
        blocks[6] = over_core(blocks[4])
        blocks[3] = over_core(blocks[1])
        blocks[5] = over_x(blocks[1])
        blocks[7] = over_core(blocks[5])

        ws = jnp.stack([wsg_loc, wsu_loc, wsd_loc.T])
        rows_s, width_s = ws.shape[1], ws.shape[2] // n_dev
        ws = ws.reshape(3, rows_s, n_dev, width_s).transpose(2, 0, 1, 3)
        ws = lax.all_to_all(ws, group_axes, 0, 0, tiled=True)

        recvs = []
        start = 0
        for n in CHUNKS:
            at = (1 - y) * n_mine + start
            piece = jnp.stack([lax.dynamic_slice_in_dim(w, at, n, 0) for w in (wg_loc, wu_loc, wdt_loc)])
            recvs.append(over_y(piece))
            start += n

        meta_rel = jnp.take(meta_all, me ^ jnp.arange(n_dev, dtype=jnp.int32), axis=0)
        ids = meta_rel[:, :top].astype(jnp.int32)
        gts = meta_rel[:, top:]
        mine = p * n_local + y * n_mine + jnp.arange(n_mine, dtype=jnp.int32)
        hit = ids[:, None] == mine[None, :, None, None]
        chosen = jnp.any(hit, axis=2).reshape(n_dev * n_mine, tok_count)
        t_ids = jnp.arange(tok_count, dtype=jnp.int32)
        before = (t_ids[:, None] < t_ids[None, :]).astype(BF16)
        rank = jnp.dot(chosen.astype(BF16), before, preferred_element_type=F32).astype(jnp.int32)
        pos = jnp.where(chosen & (rank < capacity), rank, -1)
        pos_pad = jnp.pad(pos.reshape(n_dev, n_mine, tok_count), ((0, 0), (0, TILE), (0, 0)), constant_values=-1)

        last = [pos_pad]

        def after(*vals):
            done, vals = lax.optimization_barrier((last[0], vals))
            last[0] = done
            return vals if len(vals) > 1 else vals[0]

        xg = None

        def gather(r):
            nonlocal xg
            x_blk = after(blocks[r])
            xg = gather_rows(r, n_dev, pos_pad[r], x_blk, xg, capacity)
            last[0] = xg

        base = [None] * n_dev
        shared_w = []

        def shared(r):
            if not shared_w:
                whole = after(ws).transpose(1, 0, 2, 3).reshape(3, d_model, width_s)
                shared_w.extend([whole[0], whole[1], whole[2]])
            x_blk = after(blocks[r])
            base[r] = shared_part(x_blk, *shared_w)
            last[0] = base[r]

        y_arr = y.astype(jnp.int32).reshape(1)
        outs = []

        def experts(c):
            start = sum(CHUNKS[:c])
            outs.append(expert_rows(start, CHUNKS[c], y_arr, xg, wg_loc, wu_loc, wdt_loc, after(recvs[c])))
            last[0] = outs[-1]

        lists = []

        def make_lists():
            p_in, ids_in, gts_in = after(pos, ids, gts)
            hit_in = ids_in[:, None] == mine[None, :, None, None]
            gate_of = jnp.sum(jnp.where(hit_in, gts_in[:, None], 0.0), axis=2).reshape(n_dev * n_mine, tok_count)
            same = p_in[:, None, :] == jnp.arange(capacity, dtype=jnp.int32)[None, :, None]
            toks = jnp.sum(jnp.where(same, t_ids[None, None, :] - tok_count, 0), axis=2) + tok_count
            slot_gate = jnp.sum(jnp.where(same, gate_of[:, None, :], 0.0), axis=2)
            count = jnp.sum((p_in >= 0).astype(jnp.int32), axis=1).reshape(n_dev, 1, n_mine)
            toks = (toks * TILE).reshape(n_dev, 1, n_mine * capacity)
            slot_gate = slot_gate.reshape(n_dev, 1, n_mine * capacity)
            lists.extend([count, toks, slot_gate])
            last[0] = (toks, slot_gate)

        def part(r, bases, first, halves):
            count, toks, slot_gate = lists
            c0 = 0
            while sum(CHUNKS[:c0]) < first:
                c0 += 1
            (b0, *rest) = bases
            args = [after(b0), *rest]
            out = combine(r, count[r], toks[r], slot_gate[r], args, outs[c0:], first, halves)
            last[0] = out[0] if halves else out
            return out

        gather(0)
        gather(2)
        gather(1)
        gather(4)
        gather(3)
        gather(6)
        make_lists()
        gather(5)
        gather(7)
        experts(0)
        experts(1)
        shared(7)
        shared(5)
        experts(2)
        n_pre = sum(CHUNKS[:3])
        pre7 = part(7, [base[7]], 0, False)
        pre5 = part(5, [base[5]], 0, False)
        experts(3)
        shared(6)
        experts(4)
        mate7 = over_core(part(7, [pre7], n_pre, False))
        mate6 = over_core(part(6, [base[6]], 0, False))
        diag = part(5, [pre5, mate7], n_pre, True)
        diag_x = over_x(diag[0])
        diag_y = over_y(diag[1])
        shared(4)
        to_x = part(4, [base[4], mate6], 0, True)
        x_top = over_x(to_x[0])
        shared(3)
        mate3 = over_core(part(3, [base[3]], 0, False))
        shared(1)
        to_y = part(1, [base[1], mate3], 0, True)
        y_bot = over_y(to_y[1])
        shared(2)
        mate2 = over_core(part(2, [base[2]], 0, False))
        shared(0)
        own = part(0, [base[0], mate2], 0, True)
        up_x, up_y, to_x1, to_y0 = after(diag_y, diag_x, to_x[1], to_y[0])
        x_bot = over_x(to_x1 + up_x)
        y_top = over_y(to_y0 + up_y)
        h = tok_count // 2
        top_rows = x_loc[:h].astype(F32) + own[0] + x_top + y_top
        bot_rows = x_loc[h:].astype(F32) + own[1] + x_bot + y_bot
        return jnp.concatenate([top_rows.astype(BF16), bot_rows.astype(BF16)], axis=0)

    in_specs = (tok_spec, tok_spec, tok_spec, P("expert", "data", None), P("expert", "data", None), P("expert", None, "data"), P(group_axes, None), P(group_axes, None), P(None, group_axes))
    return jax.shard_map(device_fn, mesh=mesh, in_specs=in_specs, out_specs=tok_spec, check_vma=False)
```

```python
import functools

import jax
import jax.numpy as jnp
from jax import lax
from jax.experimental import pallas as pl
from jax.experimental.pallas import tpu as pltpu
from jax.sharding import PartitionSpec as P


CAP_NUM = 5
CAP_DEN = 4
BF16 = jnp.bfloat16
F32 = jnp.float32
CHUNKS = (2, 2, 2, 1, 1)
LANES = 128
TILE = 8
VMEM_LIMIT = 56 * 1024 * 1024


SLOT = {7: 0, 5: 1, 6: 2, 4: 3, 3: 4, 1: 5, 2: 6, 0: 7}


def capacity_of(tok_count, top_count, n_exp):
    return max(8, ((CAP_NUM * top_count * tok_count) // (CAP_DEN * n_exp) + 7) // 8 * 8)


def params(sem):
    return pltpu.CompilerParams(dimension_semantics=sem, vmem_limit_bytes=VMEM_LIMIT)


def cost(flops, nbytes):
    return pl.CostEstimate(flops=int(flops) // 64, bytes_accessed=int(nbytes), transcendentals=0)


def gather_kernel(per_step, capacity, pos_ref, x_ref, *refs):
    out_ref, hot_ref = refs[-2], refs[-1]
    step = pl.program_id(0)
    tok_count = x_ref.shape[0]
    slot = lax.broadcasted_iota(jnp.int32, (capacity, tok_count), 0)
    for i in range(per_step):
        pos = pos_ref[pl.ds(step * per_step + i, 1), :]
        hot_ref[i * capacity:(i + 1) * capacity, :] = jnp.where(pos == slot, 1.0, 0.0).astype(BF16)
    rows = jnp.dot(hot_ref[...], x_ref[...], preferred_element_type=F32).astype(BF16)
    out_ref[...] = rows.reshape(out_ref.shape)


def gather_rows(slot, n_blocks, pos, x_blk, buffer, capacity):
    pos_rows, tok_count = pos.shape
    n_exp = pos_rows - TILE
    d_model = x_blk.shape[1]
    per_step = 2
    in_specs = [pl.BlockSpec((pos_rows, tok_count), lambda i: (0, 0)), pl.BlockSpec((tok_count, d_model), lambda i: (0, 0))]
    args = [pos, x_blk]
    aliases = {}
    if buffer is not None:
        in_specs.append(pl.BlockSpec(memory_space=pl.ANY))
        args.append(buffer)
        aliases = {2: 0}
    rows = n_exp * capacity
    return pl.pallas_call(
        functools.partial(gather_kernel, per_step, capacity),
        out_shape=jax.ShapeDtypeStruct((n_blocks, n_exp, capacity, d_model), BF16),
        grid=(n_exp // per_step,),
        in_specs=in_specs,
        out_specs=pl.BlockSpec((1, per_step, capacity, d_model), lambda i: (slot, i, 0, 0)),
        scratch_shapes=[pltpu.VMEM((per_step * capacity, tok_count), BF16)],
        input_output_aliases=aliases,
        compiler_params=params(("arbitrary",)),
        cost_estimate=cost(2 * rows * tok_count * d_model, rows * d_model * 2),
        name="gather_rows",
    )(*args)


def swiglu(x, w_gate, w_up, w_down_t):
    gate_pre = jnp.dot(x, w_gate, preferred_element_type=F32)
    up_pre = jnp.dot(x, w_up, preferred_element_type=F32)
    hidden = (jax.nn.silu(gate_pre) * up_pre).astype(BF16)
    return lax.dot_general(hidden, w_down_t, (((1,), (1,)), ((), ())), preferred_element_type=F32)


def expert_kernel(half, y_ref, xg_ref, og_ref, ou_ref, od_ref, rv_ref, out_ref, wg_ref, wu_ref, wd_ref):
    @pl.when(pl.program_id(1) == 0)
    def _():
        mine = pl.multiple_of(y_ref[0] * half, 64)
        other = pl.multiple_of((1 - y_ref[0]) * half, 64)
        wg_ref[pl.ds(mine, half), :] = og_ref[0]
        wu_ref[pl.ds(mine, half), :] = ou_ref[0]
        wd_ref[pl.ds(mine, half), :] = od_ref[0]
        wg_ref[pl.ds(other, half), :] = rv_ref[0, 0]
        wu_ref[pl.ds(other, half), :] = rv_ref[1, 0]
        wd_ref[pl.ds(other, half), :] = rv_ref[2, 0]

    n_blk, _, capacity, d_model = xg_ref.shape
    x = xg_ref[...].reshape(n_blk * capacity, d_model)
    out = swiglu(x, wg_ref[...], wu_ref[...], wd_ref[...])
    out_ref[...] = out.astype(BF16).reshape(out_ref.shape)


def expert_rows(first, count, slots, y_arr, xg, wg, wu, wdt, recv):
    n_exp, capacity, d_model = xg.shape[1:]
    half, width = wg.shape[1:]
    per_step = 2
    skip = slots[0] // per_step
    n_blocks = slots[1] - slots[0]
    own = pl.BlockSpec((1, half, width), lambda i, m, y: (y[0] * n_exp + first + i, 0, 0))
    return pl.pallas_call(
        functools.partial(expert_kernel, half),
        out_shape=jax.ShapeDtypeStruct((count, n_blocks, capacity, d_model), BF16),
        grid_spec=pltpu.PrefetchScalarGridSpec(
            num_scalar_prefetch=1,
            grid=(count, n_blocks // per_step),
            in_specs=[
                pl.BlockSpec((per_step, 1, capacity, d_model), lambda i, m, y: (m + skip, first + i, 0, 0)),
                own, own, own,
                pl.BlockSpec((3, 1, half, width), lambda i, m, y: (0, i, 0, 0)),
            ],
            out_specs=pl.BlockSpec((1, per_step, capacity, d_model), lambda i, m, y: (i, m, 0, 0)),
            scratch_shapes=[pltpu.VMEM((2 * half, width), BF16)] * 3,
        ),
        compiler_params=params(("arbitrary", "arbitrary")),
        cost_estimate=cost(6 * count * n_blocks * capacity * d_model * width, 4 * count * n_blocks * capacity * d_model),
        name="expert_rows",
    )(y_arr, xg, wg, wu, wdt, recv)


def shared_kernel(x_ref, wg_ref, wu_ref, wd_ref, out_ref):
    out_ref[...] = swiglu(x_ref[...], wg_ref[...], wu_ref[...], wd_ref[...])


def shared_part(x_blk, wg, wu, wdt):
    tok_count, d_model = x_blk.shape
    width = wdt.shape[1]
    tile = 512
    rows = pl.BlockSpec((tile, d_model), lambda i: (i, 0))
    return pl.pallas_call(
        shared_kernel,
        out_shape=jax.ShapeDtypeStruct((tok_count, d_model), F32),
        grid=(tok_count // tile,),
        in_specs=[rows] + [pl.BlockSpec((d_model, width), lambda i: (0, 0))] * 3,
        out_specs=rows,
        compiler_params=params(("arbitrary",)),
        cost_estimate=cost(6 * tok_count * d_model * width, 6 * tok_count * d_model),
        name="shared_part",
    )(x_blk, wg, wu, wdt)


def combine_kernel(n_base, where_of, halves, capacity, group, *refs):
    cnt_ref, tok_ref, gate_ref = refs[:3]
    bases = refs[3:3 + n_base]
    n_chunks = max(w[0] for w in where_of) + 1
    outs = refs[3 + n_base:3 + n_base + n_chunks]
    n_out = 2 if halves else 1
    pos = 3 + n_base + n_chunks
    y_refs = refs[pos:pos + n_out]
    acc, tmps, rows, wide, sem_in, sem_rows, sem_out = refs[pos + n_out:]
    tok_count, d_model = bases[0].shape
    n_col = d_model // LANES
    step = 256
    n_step = tok_count // step

    def in_copy(k, b):
        at = pl.ds(b * step, step)
        return pltpu.make_async_copy(bases[k].at[at], tmps.at[k, at], sem_in.at[k, b])

    def out_copy(b):
        at = b * step
        per_out = tok_count // n_out
        dst = y_refs[at // per_out].at[pl.ds(at % per_out, step)]
        return pltpu.make_async_copy(tmps.at[0, pl.ds(at, step)], dst, sem_out.at[b])

    def row_copy(i):
        c, local, slot, _ = where_of[i]
        return pltpu.make_async_copy(outs[c].at[local, slot], rows.at[i % 2], sem_rows.at[i % 2])

    for b in range(n_step):
        for k in range(n_base):
            in_copy(k, b).start()
    row_copy(0).start()

    for b in range(n_step):
        for k in range(n_base):
            in_copy(k, b).wait()

        @pl.loop(0, step // 32)
        def _(q):
            at = pl.multiple_of(b * step + q * 32, 32)
            val = tmps[0, pl.ds(at, 32), :]
            for k in range(1, n_base):
                val = val + tmps[k, pl.ds(at, 32), :]
            for j in range(n_col):
                acc[pl.ds(at * TILE + j, 32, stride=TILE), :] = val[:, j * LANES:(j + 1) * LANES]

    for i in range(len(where_of)):
        row_copy(i).wait()
        if i + 1 < len(where_of):
            row_copy(i + 1).start()
        e = where_of[i][3]
        slot = i % 2

        @pl.loop(0, capacity // 32)
        def _(q):
            at = pl.multiple_of(q * 32, 32)
            val = rows[slot, pl.ds(at, 32), :].astype(F32)
            for j in range(n_col):
                wide[pl.ds(at * TILE + j, 32, stride=TILE), :] = val[:, j * LANES:(j + 1) * LANES]

        @pl.loop(0, (cnt_ref[0, e] + (group - 1)) // group)
        def _(q):
            sums, toks = [], []
            for i in range(group):
                s = q * group + i
                t = tok_ref[0, e * capacity + s]
                g = gate_ref[0, e * tok_count + t]
                t = pl.multiple_of(t * TILE, TILE)
                toks.append(t)
                sums.append(acc[pl.ds(t, TILE), :] + g * wide[pl.ds(pl.multiple_of(s * TILE, TILE), TILE), :])
            for i in range(group):
                acc[pl.ds(toks[i], TILE), :] = sums[i]

    for b in range(n_step):

        @pl.loop(0, step // 32)
        def _(q):
            at = pl.multiple_of(b * step + q * 32, 32)
            for j in range(n_col):
                tmps[0, pl.ds(at, 32), j * LANES:(j + 1) * LANES] = acc[pl.ds(at * TILE + j, 32, stride=TILE), :]

        out_copy(b).start()
    for b in range(n_step):
        out_copy(b).wait()


def combine(cnt, toks, gates, bases, outs, slots, first, halves):
    tok_count, d_model = bases[0].shape
    capacity = outs[0].shape[2]
    where_of = []
    for c, o in enumerate(outs):
        for i in range(o.shape[0]):
            where_of.append((c, i, slots[c], first + len(where_of)))
    smem = pl.BlockSpec(memory_space=pltpu.SMEM)
    hbm = pl.BlockSpec(memory_space=pl.ANY)
    n_base = len(bases)
    if halves:
        out_shape = [jax.ShapeDtypeStruct((tok_count // 2, d_model), F32)] * 2
        out_specs = [hbm, hbm]
    else:
        out_shape, out_specs = jax.ShapeDtypeStruct((tok_count, d_model), F32), hbm
    return pl.pallas_call(
        functools.partial(combine_kernel, n_base, tuple(where_of), halves, capacity, 8),
        out_shape=out_shape,
        in_specs=[smem, smem, smem] + [hbm] * (n_base + len(outs)),
        out_specs=out_specs,
        scratch_shapes=[
            pltpu.VMEM(((tok_count + 1) * TILE, LANES), F32),
            pltpu.VMEM((n_base, tok_count, d_model), F32),
            pltpu.VMEM((2, capacity, d_model), BF16),
            pltpu.VMEM((capacity * TILE, LANES), F32),
            pltpu.SemaphoreType.DMA((n_base, tok_count // 256)),
            pltpu.SemaphoreType.DMA((2,)),
            pltpu.SemaphoreType.DMA((tok_count // 256,)),
        ],
        compiler_params=pltpu.CompilerParams(vmem_limit_bytes=VMEM_LIMIT),
        cost_estimate=cost(len(where_of) * capacity * tok_count * d_model, tok_count * d_model * 8),
        name="combine",
    )(cnt, toks, gates, *bases, *outs)


def finish_kernel(n_half, a_ref, b_ref, c_ref, d_ref, out_ref):
    @pl.when(pl.program_id(0) < n_half)
    def _():
        out_ref[...] = (a_ref[...] + b_ref[...]).astype(BF16)

    @pl.when(pl.program_id(0) >= n_half)
    def _():
        out_ref[...] = (c_ref[...] + d_ref[...]).astype(BF16)


def finish(top_sum, top_late, bot_sum, bot_late):
    rows, d_model = top_sum.shape
    tile = 256
    n_half = rows // tile
    top = pl.BlockSpec((tile, d_model), lambda i: (jnp.minimum(i, n_half - 1), 0))
    bot = pl.BlockSpec((tile, d_model), lambda i: (jnp.maximum(i - n_half, 0), 0))
    return pl.pallas_call(
        functools.partial(finish_kernel, n_half),
        out_shape=jax.ShapeDtypeStruct((2 * rows, d_model), BF16),
        grid=(2 * n_half,),
        in_specs=[top, top, bot, bot],
        out_specs=pl.BlockSpec((tile, d_model), lambda i: (i, 0)),
        compiler_params=params(("arbitrary",)),
        name="finish",
    )(top_sum, top_late, bot_sum, bot_late)


def solution(mesh):
    exp_n = mesh.shape["expert"]
    data_n = mesh.shape["data"]
    assert exp_n == 4 and data_n == 2
    tok_spec = P(("rep", "expert", "data"), None)
    group_axes = ("expert", "data")
    n_dev = exp_n * data_n

    def over_y(v):
        return lax.ppermute(v, "data", [(i, i ^ 1) for i in range(data_n)])

    def over_core(v):
        return lax.ppermute(v, "expert", [(i, i ^ 1) for i in range(exp_n)])

    def over_x(v):
        return lax.ppermute(v, "expert", [(i, i ^ 2) for i in range(exp_n)])

    def over_all(v, r):
        flip = (r & 1) * exp_n + (r >> 1)
        return lax.ppermute(v, ("data", "expert"), [(i, i ^ flip) for i in range(n_dev)])

    def device_fn(x_loc, idx_loc, gate_loc, wg_loc, wu_loc, wd_loc, wsg_loc, wsu_loc, wsd_loc):
        tok_count, d_model = x_loc.shape
        top = idx_loc.shape[1]
        n_local, _, _ = wg_loc.shape
        n_mine = n_local // data_n
        capacity = capacity_of(tok_count, top, n_local * exp_n)
        y = lax.axis_index("data")
        p = lax.axis_index("expert")
        wdt_loc = jnp.swapaxes(wd_loc, 1, 2)

        meta = jnp.concatenate([idx_loc.T.astype(F32), gate_loc.T], axis=0)
        meta_rel = [meta]
        for r in range(1, n_dev):
            meta_rel.append(over_all(meta, r))

        blocks = [None] * n_dev
        blocks[0] = x_loc
        blocks[1] = over_y(x_loc)
        blocks[4] = over_x(x_loc)
        blocks[2] = over_core(x_loc)
        blocks[6] = over_core(blocks[4])
        blocks[3] = over_core(blocks[1])
        blocks[5] = over_x(blocks[1])
        blocks[7] = over_core(blocks[5])

        ws = jnp.stack([wsg_loc, wsu_loc, wsd_loc.T])
        rows_s, width_s = ws.shape[1], ws.shape[2] // n_dev
        ws = ws.reshape(3, rows_s, n_dev, width_s).transpose(2, 0, 1, 3)
        by_rel = (p * data_n + y) ^ jnp.arange(n_dev, dtype=jnp.int32)
        ws = jnp.take(ws, by_rel, axis=0)
        ws_parts = [ws[0]]
        for r in range(1, n_dev):
            ws_parts.append(over_all(ws[r], r))

        recvs = []
        start = 0
        for n in CHUNKS:
            at = (1 - y) * n_mine + start
            piece = jnp.stack([lax.dynamic_slice_in_dim(w, at, n, 0) for w in (wg_loc, wu_loc, wdt_loc)])
            recvs.append(over_y(piece))
            start += n

        meta_rel = jnp.stack(meta_rel)
        ids = meta_rel[:, :top].astype(jnp.int32)
        gts = meta_rel[:, top:]
        mine = p * n_local + y * n_mine + jnp.arange(n_mine, dtype=jnp.int32)
        hit = ids[:, None] == mine[None, :, None, None]
        chosen = jnp.any(hit, axis=2).reshape(n_dev * n_mine, tok_count)
        t_ids = jnp.arange(tok_count, dtype=jnp.int32)
        before = (t_ids[:, None] < t_ids[None, :]).astype(BF16)
        rank = jnp.dot(chosen.astype(BF16), before, preferred_element_type=F32).astype(jnp.int32)
        pos = jnp.where(chosen & (rank < capacity), rank, -1)
        pos_pad = jnp.pad(pos.reshape(n_dev, n_mine, tok_count), ((0, 0), (0, TILE), (0, 0)), constant_values=-1)

        last = [pos_pad]

        def after(*vals):
            done, vals = lax.optimization_barrier((last[0], vals))
            last[0] = done
            return vals if len(vals) > 1 else vals[0]

        xg = None

        def gather(r):
            nonlocal xg
            x_blk = after(blocks[r])
            xg = gather_rows(SLOT[r], n_dev, pos_pad[r], x_blk, xg, capacity)
            last[0] = xg

        base = [None] * n_dev
        shared_w = []

        def shared(r):
            if not shared_w:
                whole = jnp.take(jnp.stack(after(*ws_parts)), by_rel, axis=0)
                whole = whole.transpose(1, 0, 2, 3).reshape(3, d_model, width_s)
                shared_w.extend([whole[0], whole[1], whole[2]])
            x_blk = after(blocks[r])
            base[r] = shared_part(x_blk, *shared_w)
            last[0] = base[r]

        y_arr = y.astype(jnp.int32).reshape(1)

        def experts(c, slots=(0, n_dev)):
            start = sum(CHUNKS[:c])
            recv = after(recvs[c])
            out = expert_rows(start, CHUNKS[c], slots, y_arr, xg, wg_loc, wu_loc, wdt_loc, recv)
            last[0] = out
            return out

        lists = []

        def make_lists():
            p_in, ids_in, gts_in = after(pos, ids, gts)
            hit_in = ids_in[:, None] == mine[None, :, None, None]
            gate_of = jnp.sum(jnp.where(hit_in, gts_in[:, None], 0.0), axis=2).reshape(n_dev, 1, n_mine * tok_count)
            gate_of = jnp.pad(gate_of, ((0, 0), (0, 0), (0, LANES)))
            same = p_in[:, None, :] == jnp.arange(capacity, dtype=jnp.int32)[None, :, None]
            toks = jnp.sum(jnp.where(same, t_ids[None, None, :] - tok_count, 0), axis=2) + tok_count
            count = jnp.sum((p_in >= 0).astype(jnp.int32), axis=1).reshape(n_dev, 1, n_mine)
            toks = toks.reshape(n_dev, 1, n_mine * capacity)
            lists.extend([count, toks, gate_of])
            last[0] = (toks, gate_of)

        def part(r, bases, arrays, first, halves):
            count, toks, gate_of = lists
            outs_r = [o for o, _ in arrays]
            slots_r = [SLOT[r] - s0 for _, s0 in arrays]
            (b0, *rest) = bases
            args = [after(b0), *rest]
            out = combine(count[r], toks[r], gate_of[r], args, outs_r, slots_r, first, halves)
            last[0] = out[0] if halves else out
            return out

        gather(0)
        gather(2)
        gather(1)
        gather(4)
        gather(3)
        gather(6)
        make_lists()
        gather(5)
        gather(7)
        early = [(experts(0), 0), (experts(1), 0)]
        shared(7)
        shared(5)
        early.append((experts(2), 0))
        n_pre = sum(CHUNKS[:3])
        pre7 = part(7, [base[7]], early, 0, False)
        pre5 = part(5, [base[5]], early, 0, False)
        early.append((experts(3), 0))
        shared(6)
        pre6 = part(6, [base[6]], early, 0, False)
        shared(4)
        shared(3)
        tail = experts(4, (0, 2))
        late = [early[3], (tail, 0)]
        mate7 = over_core(part(7, [pre7], late, n_pre, False))
        rest = experts(4, (2, n_dev))
        full = early + [(rest, 2)]
        diag = part(5, [pre5, mate7], late, n_pre, True)
        diag_x = over_x(diag[0])
        diag_y = over_y(diag[1])
        mate6 = over_core(part(6, [pre6], [(rest, 2)], n_pre + CHUNKS[3], False))
        mate3 = over_core(part(3, [base[3]], full, 0, False))
        to_x = part(4, [base[4], mate6], full, 0, True)
        x_top = over_x(to_x[0])
        shared(1)
        to_y = part(1, [base[1], mate3], full, 0, True)
        y_bot = over_y(to_y[1])
        shared(2)
        mate2 = over_core(part(2, [base[2]], full, 0, False))
        shared(0)
        own = part(0, [base[0], mate2], full, 0, True)
        up_x, up_y, to_x1, to_y0 = after(diag_y, diag_x, to_x[1], to_y[0])
        x_bot = over_x(to_x1 + up_x)
        y_top = over_y(to_y0 + up_y)
        h = tok_count // 2
        sum_top = x_loc[:h].astype(F32) + own[0] + x_top
        sum_bot = x_loc[h:].astype(F32) + own[1] + y_bot
        sum_top, sum_bot = lax.optimization_barrier((sum_top, sum_bot))
        return finish(sum_top, y_top, sum_bot, x_bot)

    in_specs = (tok_spec, tok_spec, tok_spec, P("expert", "data", None), P("expert", "data", None), P("expert", None, "data"), P(group_axes, None), P(group_axes, None), P(None, group_axes))
    return jax.shard_map(device_fn, mesh=mesh, in_specs=in_specs, out_specs=tok_spec, check_vma=False)
```

```python
import functools

import jax
import jax.numpy as jnp
from jax import lax
from jax.experimental import pallas as pl
from jax.experimental.pallas import tpu as pltpu
from jax.sharding import PartitionSpec as P


CAP_NUM = 5
CAP_DEN = 4
BF16 = jnp.bfloat16
F32 = jnp.float32
CHUNKS = (2, 2, 2, 1, 1)
LANES = 128
TILE = 8
VMEM_LIMIT = 56 * 1024 * 1024


SLOT = {7: 0, 5: 1, 6: 2, 4: 3, 3: 4, 1: 5, 2: 6, 0: 7}


def capacity_of(tok_count, top_count, n_exp):
    return max(8, ((CAP_NUM * top_count * tok_count) // (CAP_DEN * n_exp) + 7) // 8 * 8)


def params(sem):
    return pltpu.CompilerParams(dimension_semantics=sem, vmem_limit_bytes=VMEM_LIMIT)


def cost(flops, nbytes):
    return pl.CostEstimate(flops=int(flops) // 64, bytes_accessed=int(nbytes), transcendentals=0)


def gather_kernel(per_step, capacity, pos_ref, x_ref, *refs):
    out_ref, hot_ref = refs[-2], refs[-1]
    step = pl.program_id(0)
    tok_count = x_ref.shape[0]
    slot = lax.broadcasted_iota(jnp.int32, (capacity, tok_count), 0)
    for i in range(per_step):
        pos = pos_ref[pl.ds(step * per_step + i, 1), :]
        hot_ref[i * capacity:(i + 1) * capacity, :] = jnp.where(pos == slot, 1.0, 0.0).astype(BF16)
    rows = jnp.dot(hot_ref[...], x_ref[...], preferred_element_type=F32).astype(BF16)
    out_ref[...] = rows.reshape(out_ref.shape)


def gather_rows(slot, n_blocks, pos, x_blk, buffer, capacity):
    pos_rows, tok_count = pos.shape
    n_exp = pos_rows - TILE
    d_model = x_blk.shape[1]
    per_step = 2
    in_specs = [pl.BlockSpec((pos_rows, tok_count), lambda i: (0, 0)), pl.BlockSpec((tok_count, d_model), lambda i: (0, 0))]
    args = [pos, x_blk]
    aliases = {}
    if buffer is not None:
        in_specs.append(pl.BlockSpec(memory_space=pl.ANY))
        args.append(buffer)
        aliases = {2: 0}
    rows = n_exp * capacity
    return pl.pallas_call(
        functools.partial(gather_kernel, per_step, capacity),
        out_shape=jax.ShapeDtypeStruct((n_blocks, n_exp, capacity, d_model), BF16),
        grid=(n_exp // per_step,),
        in_specs=in_specs,
        out_specs=pl.BlockSpec((1, per_step, capacity, d_model), lambda i: (slot, i, 0, 0)),
        scratch_shapes=[pltpu.VMEM((per_step * capacity, tok_count), BF16)],
        input_output_aliases=aliases,
        compiler_params=params(("arbitrary",)),
        cost_estimate=cost(2 * rows * tok_count * d_model, rows * d_model * 2),
        name="gather_rows",
    )(*args)


def swiglu(x, w_gate, w_up, w_down_t):
    gate_pre = jnp.dot(x, w_gate, preferred_element_type=F32)
    up_pre = jnp.dot(x, w_up, preferred_element_type=F32)
    hidden = (jax.nn.silu(gate_pre) * up_pre).astype(BF16)
    return lax.dot_general(hidden, w_down_t, (((1,), (1,)), ((), ())), preferred_element_type=F32)


def expert_kernel(half, y_ref, xg_ref, og_ref, ou_ref, od_ref, rv_ref, out_ref, wg_ref, wu_ref, wd_ref):
    @pl.when(pl.program_id(1) == 0)
    def _():
        mine = pl.multiple_of(y_ref[0] * half, 64)
        other = pl.multiple_of((1 - y_ref[0]) * half, 64)
        wg_ref[pl.ds(mine, half), :] = og_ref[0]
        wu_ref[pl.ds(mine, half), :] = ou_ref[0]
        wd_ref[pl.ds(mine, half), :] = od_ref[0]
        wg_ref[pl.ds(other, half), :] = rv_ref[0, 0]
        wu_ref[pl.ds(other, half), :] = rv_ref[1, 0]
        wd_ref[pl.ds(other, half), :] = rv_ref[2, 0]

    n_blk, _, capacity, d_model = xg_ref.shape
    x = xg_ref[...].reshape(n_blk * capacity, d_model)
    out = swiglu(x, wg_ref[...], wu_ref[...], wd_ref[...])
    out_ref[...] = out.astype(BF16).reshape(out_ref.shape)


def expert_rows(first, count, slots, y_arr, xg, wg, wu, wdt, recv):
    n_exp, capacity, d_model = xg.shape[1:]
    half, width = wg.shape[1:]
    per_step = 2
    skip = slots[0] // per_step
    n_blocks = slots[1] - slots[0]
    own = pl.BlockSpec((1, half, width), lambda i, m, y: (y[0] * n_exp + first + i, 0, 0))
    return pl.pallas_call(
        functools.partial(expert_kernel, half),
        out_shape=jax.ShapeDtypeStruct((count, n_blocks, capacity, d_model), BF16),
        grid_spec=pltpu.PrefetchScalarGridSpec(
            num_scalar_prefetch=1,
            grid=(count, n_blocks // per_step),
            in_specs=[
                pl.BlockSpec((per_step, 1, capacity, d_model), lambda i, m, y: (m + skip, first + i, 0, 0)),
                own, own, own,
                pl.BlockSpec((3, 1, half, width), lambda i, m, y: (0, i, 0, 0)),
            ],
            out_specs=pl.BlockSpec((1, per_step, capacity, d_model), lambda i, m, y: (i, m, 0, 0)),
            scratch_shapes=[pltpu.VMEM((2 * half, width), BF16)] * 3,
        ),
        compiler_params=params(("arbitrary", "arbitrary")),
        cost_estimate=cost(6 * count * n_blocks * capacity * d_model * width, 4 * count * n_blocks * capacity * d_model),
        name="expert_rows",
    )(y_arr, xg, wg, wu, wdt, recv)


def shared_kernel(x_ref, w_ref, out_ref):
    out_ref[...] = swiglu(x_ref[...], w_ref[0], w_ref[1], w_ref[2])


def shared_part(x_blk, w_all):
    tok_count, d_model = x_blk.shape
    width = w_all.shape[2]
    tile = 512
    rows = pl.BlockSpec((tile, d_model), lambda i: (i, 0))
    return pl.pallas_call(
        shared_kernel,
        out_shape=jax.ShapeDtypeStruct((tok_count, d_model), F32),
        grid=(tok_count // tile,),
        in_specs=[rows, pl.BlockSpec((3, d_model, width), lambda i: (0, 0, 0))],
        out_specs=rows,
        compiler_params=params(("arbitrary",)),
        cost_estimate=cost(6 * tok_count * d_model * width, 6 * tok_count * d_model),
        name="shared_part",
    )(x_blk, w_all)


def combine_kernel(n_base, where_of, halves, capacity, group, *refs):
    cnt_ref, tok_ref, gate_ref = refs[:3]
    bases = refs[3:3 + n_base]
    n_chunks = max(w[0] for w in where_of) + 1
    outs = refs[3 + n_base:3 + n_base + n_chunks]
    n_out = 2 if halves else 1
    pos = 3 + n_base + n_chunks
    y_refs = refs[pos:pos + n_out]
    acc, tmps, rows, wide, sem_in, sem_rows, sem_out = refs[pos + n_out:]
    tok_count, d_model = bases[0].shape
    n_col = d_model // LANES
    step = 256
    n_step = tok_count // step

    def in_copy(k, b):
        at = pl.ds(b * step, step)
        return pltpu.make_async_copy(bases[k].at[at], tmps.at[k, at], sem_in.at[k, b])

    def out_copy(b):
        at = b * step
        per_out = tok_count // n_out
        dst = y_refs[at // per_out].at[pl.ds(at % per_out, step)]
        return pltpu.make_async_copy(tmps.at[0, pl.ds(at, step)], dst, sem_out.at[b])

    def row_copy(i):
        c, local, slot, _ = where_of[i]
        return pltpu.make_async_copy(outs[c].at[local, slot], rows.at[i % 2], sem_rows.at[i % 2])

    for b in range(n_step):
        for k in range(n_base):
            in_copy(k, b).start()
    row_copy(0).start()

    for b in range(n_step):
        for k in range(n_base):
            in_copy(k, b).wait()

        @pl.loop(0, step // 32)
        def _(q):
            at = pl.multiple_of(b * step + q * 32, 32)
            val = tmps[0, pl.ds(at, 32), :]
            for k in range(1, n_base):
                val = val + tmps[k, pl.ds(at, 32), :]
            for j in range(n_col):
                acc[pl.ds(at * TILE + j, 32, stride=TILE), :] = val[:, j * LANES:(j + 1) * LANES]

    for i in range(len(where_of)):
        row_copy(i).wait()
        if i + 1 < len(where_of):
            row_copy(i + 1).start()
        e = where_of[i][3]
        slot = i % 2

        @pl.loop(0, capacity // 32)
        def _(q):
            at = pl.multiple_of(q * 32, 32)
            val = rows[slot, pl.ds(at, 32), :].astype(F32)
            for j in range(n_col):
                wide[pl.ds(at * TILE + j, 32, stride=TILE), :] = val[:, j * LANES:(j + 1) * LANES]

        @pl.loop(0, (cnt_ref[0, e] + (group - 1)) // group)
        def _(q):
            sums, toks = [], []
            for i in range(group):
                s = q * group + i
                t = tok_ref[0, e * capacity + s]
                g = gate_ref[0, e * tok_count + t]
                t = pl.multiple_of(t * TILE, TILE)
                toks.append(t)
                sums.append(acc[pl.ds(t, TILE), :] + g * wide[pl.ds(pl.multiple_of(s * TILE, TILE), TILE), :])
            for i in range(group):
                acc[pl.ds(toks[i], TILE), :] = sums[i]

    for b in range(n_step):

        @pl.loop(0, step // 32)
        def _(q):
            at = pl.multiple_of(b * step + q * 32, 32)
            for j in range(n_col):
                tmps[0, pl.ds(at, 32), j * LANES:(j + 1) * LANES] = acc[pl.ds(at * TILE + j, 32, stride=TILE), :]

        out_copy(b).start()
    for b in range(n_step):
        out_copy(b).wait()


def combine(cnt, toks, gates, bases, outs, slots, first, halves):
    tok_count, d_model = bases[0].shape
    capacity = outs[0].shape[2]
    where_of = []
    for c, o in enumerate(outs):
        for i in range(o.shape[0]):
            where_of.append((c, i, slots[c], first + len(where_of)))
    smem = pl.BlockSpec(memory_space=pltpu.SMEM)
    hbm = pl.BlockSpec(memory_space=pl.ANY)
    n_base = len(bases)
    if halves:
        out_shape = [jax.ShapeDtypeStruct((tok_count // 2, d_model), F32)] * 2
        out_specs = [hbm, hbm]
    else:
        out_shape, out_specs = jax.ShapeDtypeStruct((tok_count, d_model), F32), hbm
    return pl.pallas_call(
        functools.partial(combine_kernel, n_base, tuple(where_of), halves, capacity, 8),
        out_shape=out_shape,
        in_specs=[smem, smem, smem] + [hbm] * (n_base + len(outs)),
        out_specs=out_specs,
        scratch_shapes=[
            pltpu.VMEM(((tok_count + 1) * TILE, LANES), F32),
            pltpu.VMEM((n_base, tok_count, d_model), F32),
            pltpu.VMEM((2, capacity, d_model), BF16),
            pltpu.VMEM((capacity * TILE, LANES), F32),
            pltpu.SemaphoreType.DMA((n_base, tok_count // 256)),
            pltpu.SemaphoreType.DMA((2,)),
            pltpu.SemaphoreType.DMA((tok_count // 256,)),
        ],
        compiler_params=pltpu.CompilerParams(vmem_limit_bytes=VMEM_LIMIT),
        cost_estimate=cost(len(where_of) * capacity * tok_count * d_model, tok_count * d_model * 8),
        name="combine",
    )(cnt, toks, gates, *bases, *outs)


def assemble_kernel(me_ref, *refs):
    out_ref = refs[-1]
    for r, part in enumerate(refs[:-1]):
        rows = part.shape[1]
        at = pl.multiple_of((me_ref[0] ^ r) * rows, 16)
        for k in range(part.shape[0]):
            out_ref[k, pl.ds(at, rows), :] = part[k]


def assemble(me_arr, parts):
    n_arr, rows, width = parts[0].shape
    vmem = pl.BlockSpec(memory_space=pltpu.VMEM)
    return pl.pallas_call(
        assemble_kernel,
        out_shape=jax.ShapeDtypeStruct((n_arr, len(parts) * rows, width), BF16),
        in_specs=[pl.BlockSpec(memory_space=pltpu.SMEM)] + [vmem] * len(parts),
        out_specs=vmem,
        compiler_params=pltpu.CompilerParams(vmem_limit_bytes=VMEM_LIMIT),
        name="assemble",
    )(me_arr, *parts)


def finish_kernel(n_half, a_ref, b_ref, c_ref, d_ref, out_ref):
    @pl.when(pl.program_id(0) < n_half)
    def _():
        out_ref[...] = (a_ref[...] + b_ref[...]).astype(BF16)

    @pl.when(pl.program_id(0) >= n_half)
    def _():
        out_ref[...] = (c_ref[...] + d_ref[...]).astype(BF16)


def finish(top_sum, top_late, bot_sum, bot_late):
    rows, d_model = top_sum.shape
    tile = 256
    n_half = rows // tile
    top = pl.BlockSpec((tile, d_model), lambda i: (jnp.minimum(i, n_half - 1), 0))
    bot = pl.BlockSpec((tile, d_model), lambda i: (jnp.maximum(i - n_half, 0), 0))
    return pl.pallas_call(
        functools.partial(finish_kernel, n_half),
        out_shape=jax.ShapeDtypeStruct((2 * rows, d_model), BF16),
        grid=(2 * n_half,),
        in_specs=[top, top, bot, bot],
        out_specs=pl.BlockSpec((tile, d_model), lambda i: (i, 0)),
        compiler_params=params(("arbitrary",)),
        name="finish",
    )(top_sum, top_late, bot_sum, bot_late)


def solution(mesh):
    exp_n = mesh.shape["expert"]
    data_n = mesh.shape["data"]
    assert exp_n == 4 and data_n == 2
    tok_spec = P(("rep", "expert", "data"), None)
    group_axes = ("expert", "data")
    n_dev = exp_n * data_n

    def over_y(v):
        return lax.ppermute(v, "data", [(i, i ^ 1) for i in range(data_n)])

    def over_core(v):
        return lax.ppermute(v, "expert", [(i, i ^ 1) for i in range(exp_n)])

    def over_x(v):
        return lax.ppermute(v, "expert", [(i, i ^ 2) for i in range(exp_n)])

    def over_all(v, r):
        flip = (r & 1) * exp_n + (r >> 1)
        return lax.ppermute(v, ("data", "expert"), [(i, i ^ flip) for i in range(n_dev)])

    def device_fn(x_loc, idx_loc, gate_loc, wg_loc, wu_loc, wd_loc, wsg_loc, wsu_loc, wsd_loc):
        tok_count, _ = x_loc.shape
        top = idx_loc.shape[1]
        n_local, _, _ = wg_loc.shape
        n_mine = n_local // data_n
        capacity = capacity_of(tok_count, top, n_local * exp_n)
        y = lax.axis_index("data")
        p = lax.axis_index("expert")
        wdt_loc = jnp.swapaxes(wd_loc, 1, 2)

        meta = jnp.concatenate([idx_loc.T.astype(F32), gate_loc.T], axis=0)
        meta_rel = [meta]
        for r in range(1, n_dev):
            meta_rel.append(over_all(meta, r))

        blocks = [None] * n_dev
        blocks[0] = x_loc
        blocks[1] = over_y(x_loc)
        blocks[4] = over_x(x_loc)
        blocks[2] = over_core(x_loc)
        blocks[6] = over_core(blocks[4])
        blocks[3] = over_core(blocks[1])
        blocks[5] = over_x(blocks[1])
        blocks[7] = over_core(blocks[5])

        ws = jnp.stack([wsg_loc, wsu_loc, wsd_loc.T])
        rows_s, width_s = ws.shape[1], ws.shape[2] // n_dev
        ws = ws.reshape(3, rows_s, n_dev, width_s).transpose(2, 0, 1, 3)
        by_rel = (p * data_n + y) ^ jnp.arange(n_dev, dtype=jnp.int32)
        ws = jnp.take(ws, by_rel, axis=0)
        ws_parts = [ws[0]]
        for r in range(1, n_dev):
            ws_parts.append(over_all(ws[r], r))

        recvs = []
        start = 0
        for n in CHUNKS:
            at = (1 - y) * n_mine + start
            piece = jnp.stack([lax.dynamic_slice_in_dim(w, at, n, 0) for w in (wg_loc, wu_loc, wdt_loc)])
            recvs.append(over_y(piece))
            start += n

        meta_rel = jnp.stack(meta_rel)
        ids = meta_rel[:, :top].astype(jnp.int32)
        gts = meta_rel[:, top:]
        mine = p * n_local + y * n_mine + jnp.arange(n_mine, dtype=jnp.int32)
        hit = ids[:, None] == mine[None, :, None, None]
        chosen = jnp.any(hit, axis=2).reshape(n_dev * n_mine, tok_count)
        t_ids = jnp.arange(tok_count, dtype=jnp.int32)
        before = (t_ids[:, None] < t_ids[None, :]).astype(BF16)
        rank = jnp.dot(chosen.astype(BF16), before, preferred_element_type=F32).astype(jnp.int32)
        pos = jnp.where(chosen & (rank < capacity), rank, -1)
        pos_pad = jnp.pad(pos.reshape(n_dev, n_mine, tok_count), ((0, 0), (0, TILE), (0, 0)), constant_values=-1)

        last = [pos_pad]

        def after(*vals):
            done, vals = lax.optimization_barrier((last[0], vals))
            last[0] = done
            return vals if len(vals) > 1 else vals[0]

        xg = None

        def gather(r):
            nonlocal xg
            x_blk = after(blocks[r])
            xg = gather_rows(SLOT[r], n_dev, pos_pad[r], x_blk, xg, capacity)
            last[0] = xg

        base = [None] * n_dev
        shared_w = []

        def shared(r):
            if not shared_w:
                whole = assemble(by_rel[:1], after(*ws_parts))
                last[0] = whole
                shared_w.append(whole)
            x_blk = after(blocks[r])
            base[r] = shared_part(x_blk, *shared_w)
            last[0] = base[r]

        y_arr = y.astype(jnp.int32).reshape(1)

        def experts(c, slots=(0, n_dev)):
            start = sum(CHUNKS[:c])
            recv = after(recvs[c])
            out = expert_rows(start, CHUNKS[c], slots, y_arr, xg, wg_loc, wu_loc, wdt_loc, recv)
            last[0] = out
            return out

        lists = []

        def make_lists():
            p_in, ids_in, gts_in = after(pos, ids, gts)
            hit_in = ids_in[:, None] == mine[None, :, None, None]
            gate_of = jnp.sum(jnp.where(hit_in, gts_in[:, None], 0.0), axis=2).reshape(n_dev, 1, n_mine * tok_count)
            gate_of = jnp.pad(gate_of, ((0, 0), (0, 0), (0, LANES)))
            same = p_in[:, None, :] == jnp.arange(capacity, dtype=jnp.int32)[None, :, None]
            toks = jnp.sum(jnp.where(same, t_ids[None, None, :] - tok_count, 0), axis=2) + tok_count
            count = jnp.sum((p_in >= 0).astype(jnp.int32), axis=1).reshape(n_dev, 1, n_mine)
            toks = toks.reshape(n_dev, 1, n_mine * capacity)
            lists.extend([count, toks, gate_of])
            last[0] = (toks, gate_of)

        def part(r, bases, arrays, first, halves):
            count, toks, gate_of = lists
            outs_r = [o for o, _ in arrays]
            slots_r = [SLOT[r] - s0 for _, s0 in arrays]
            (b0, *rest) = bases
            args = [after(b0), *rest]
            out = combine(count[r], toks[r], gate_of[r], args, outs_r, slots_r, first, halves)
            last[0] = out[0] if halves else out
            return out

        gather(0)
        gather(2)
        gather(1)
        gather(4)
        gather(3)
        gather(6)
        make_lists()
        gather(5)
        gather(7)
        early = [(experts(0), 0), (experts(1), 0)]
        shared(7)
        shared(5)
        early.append((experts(2), 0))
        n_pre = sum(CHUNKS[:3])
        pre7 = part(7, [base[7]], early, 0, False)
        pre5 = part(5, [base[5]], early, 0, False)
        early.append((experts(3), 0))
        shared(6)
        tail = experts(4, (0, 2))
        late = [early[3], (tail, 0)]
        mate7 = over_core(part(7, [pre7], late, n_pre, False))
        rest = experts(4, (2, n_dev))
        full = early + [(rest, 2)]
        diag = part(5, [pre5, mate7], late, n_pre, True)
        diag_x = over_x(diag[0])
        diag_y = over_y(diag[1])
        mate6 = over_core(part(6, [base[6]], full, 0, False))
        shared(4)
        shared(3)
        to_x = part(4, [base[4], mate6], full, 0, True)
        x_top = over_x(to_x[0])
        mate3 = over_core(part(3, [base[3]], full, 0, False))
        shared(1)
        to_y = part(1, [base[1], mate3], full, 0, True)
        y_bot = over_y(to_y[1])
        shared(2)
        mate2 = over_core(part(2, [base[2]], full, 0, False))
        shared(0)
        own = part(0, [base[0], mate2], full, 0, True)
        up_x, up_y, to_x1, to_y0 = after(diag_y, diag_x, to_x[1], to_y[0])
        x_bot = over_x(to_x1 + up_x)
        y_top = over_y(to_y0 + up_y)
        h = tok_count // 2
        sum_top = x_loc[:h].astype(F32) + own[0] + x_top
        sum_bot = x_loc[h:].astype(F32) + own[1] + y_bot
        sum_top, sum_bot = lax.optimization_barrier((sum_top, sum_bot))
        return finish(sum_top, y_top, sum_bot, x_bot)

    in_specs = (tok_spec, tok_spec, tok_spec, P("expert", "data", None), P("expert", "data", None), P("expert", None, "data"), P(group_axes, None), P(group_axes, None), P(None, group_axes))
    return jax.shard_map(device_fn, mesh=mesh, in_specs=in_specs, out_specs=tok_spec, check_vma=False)
```

```python
import functools

import jax
import jax.numpy as jnp
from jax import lax
from jax.experimental import pallas as pl
from jax.experimental.pallas import tpu as pltpu
from jax.sharding import PartitionSpec as P


CAP_NUM = 5
CAP_DEN = 4
BF16 = jnp.bfloat16
F32 = jnp.float32
CHUNKS = (2, 2, 2, 1, 1)
LANES = 128
TILE = 8
VMEM_LIMIT = 56 * 1024 * 1024


SLOT = {7: 0, 5: 1, 6: 2, 4: 3, 3: 4, 1: 5, 2: 6, 0: 7}


def capacity_of(tok_count, top_count, n_exp):
    return max(8, ((CAP_NUM * top_count * tok_count) // (CAP_DEN * n_exp) + 7) // 8 * 8)


def params(sem):
    return pltpu.CompilerParams(dimension_semantics=sem, vmem_limit_bytes=VMEM_LIMIT)


def cost(flops, nbytes):
    return pl.CostEstimate(flops=int(flops) // 64, bytes_accessed=int(nbytes), transcendentals=0)


def gather_kernel(per_step, capacity, pos_ref, x_ref, *refs):
    out_ref, hot_ref = refs[-2], refs[-1]
    step = pl.program_id(0)
    tok_count = x_ref.shape[0]
    slot = lax.broadcasted_iota(jnp.int32, (capacity, tok_count), 0)
    for i in range(per_step):
        pos = pos_ref[pl.ds(step * per_step + i, 1), :]
        hot_ref[i * capacity:(i + 1) * capacity, :] = jnp.where(pos == slot, 1.0, 0.0).astype(BF16)
    rows = jnp.dot(hot_ref[...], x_ref[...], preferred_element_type=F32).astype(BF16)
    out_ref[...] = rows.reshape(out_ref.shape)


def gather_rows(slot, n_blocks, pos, x_blk, buffer, capacity):
    pos_rows, tok_count = pos.shape
    n_exp = pos_rows - TILE
    d_model = x_blk.shape[1]
    per_step = 2
    in_specs = [pl.BlockSpec((pos_rows, tok_count), lambda i: (0, 0)), pl.BlockSpec((tok_count, d_model), lambda i: (0, 0))]
    args = [pos, x_blk]
    aliases = {}
    if buffer is not None:
        in_specs.append(pl.BlockSpec(memory_space=pl.ANY))
        args.append(buffer)
        aliases = {2: 0}
    rows = n_exp * capacity
    return pl.pallas_call(
        functools.partial(gather_kernel, per_step, capacity),
        out_shape=jax.ShapeDtypeStruct((n_blocks, n_exp, capacity, d_model), BF16),
        grid=(n_exp // per_step,),
        in_specs=in_specs,
        out_specs=pl.BlockSpec((1, per_step, capacity, d_model), lambda i: (slot, i, 0, 0)),
        scratch_shapes=[pltpu.VMEM((per_step * capacity, tok_count), BF16)],
        input_output_aliases=aliases,
        compiler_params=params(("arbitrary",)),
        cost_estimate=cost(2 * rows * tok_count * d_model, rows * d_model * 2),
        name="gather_rows",
    )(*args)


def swiglu(x, w_gate, w_up, w_down_t):
    gate_pre = jnp.dot(x, w_gate, preferred_element_type=F32)
    up_pre = jnp.dot(x, w_up, preferred_element_type=F32)
    hidden = (jax.nn.silu(gate_pre) * up_pre).astype(BF16)
    return lax.dot_general(hidden, w_down_t, (((1,), (1,)), ((), ())), preferred_element_type=F32)


def expert_kernel(half, y_ref, xg_ref, og_ref, ou_ref, od_ref, rv_ref, out_ref, wg_ref, wu_ref, wd_ref):
    @pl.when(pl.program_id(1) == 0)
    def _():
        mine = pl.multiple_of(y_ref[0] * half, 64)
        other = pl.multiple_of((1 - y_ref[0]) * half, 64)
        wg_ref[pl.ds(mine, half), :] = og_ref[0]
        wu_ref[pl.ds(mine, half), :] = ou_ref[0]
        wd_ref[pl.ds(mine, half), :] = od_ref[0]
        wg_ref[pl.ds(other, half), :] = rv_ref[0, 0]
        wu_ref[pl.ds(other, half), :] = rv_ref[1, 0]
        wd_ref[pl.ds(other, half), :] = rv_ref[2, 0]

    n_blk, _, capacity, d_model = xg_ref.shape
    x = xg_ref[...].reshape(n_blk * capacity, d_model)
    out = swiglu(x, wg_ref[...], wu_ref[...], wd_ref[...])
    out_ref[...] = out.astype(BF16).reshape(out_ref.shape)


def expert_rows(first, count, slots, y_arr, xg, wg, wu, wdt, recv):
    n_exp, capacity, d_model = xg.shape[1:]
    half, width = wg.shape[1:]
    per_step = 2
    skip = slots[0] // per_step
    n_blocks = slots[1] - slots[0]
    own = pl.BlockSpec((1, half, width), lambda i, m, y: (y[0] * n_exp + first + i, 0, 0))
    return pl.pallas_call(
        functools.partial(expert_kernel, half),
        out_shape=jax.ShapeDtypeStruct((count, n_blocks, capacity, d_model), BF16),
        grid_spec=pltpu.PrefetchScalarGridSpec(
            num_scalar_prefetch=1,
            grid=(count, n_blocks // per_step),
            in_specs=[
                pl.BlockSpec((per_step, 1, capacity, d_model), lambda i, m, y: (m + skip, first + i, 0, 0)),
                own, own, own,
                pl.BlockSpec((3, 1, half, width), lambda i, m, y: (0, i, 0, 0)),
            ],
            out_specs=pl.BlockSpec((1, per_step, capacity, d_model), lambda i, m, y: (i, m, 0, 0)),
            scratch_shapes=[pltpu.VMEM((2 * half, width), BF16)] * 3,
        ),
        compiler_params=params(("arbitrary", "arbitrary")),
        cost_estimate=cost(6 * count * n_blocks * capacity * d_model * width, 4 * count * n_blocks * capacity * d_model),
        name="expert_rows",
    )(y_arr, xg, wg, wu, wdt, recv)


def shared_kernel(x_ref, w_ref, out_ref):
    out_ref[...] = swiglu(x_ref[...], w_ref[0], w_ref[1], w_ref[2])


def shared_part(x_blk, w_all):
    tok_count, d_model = x_blk.shape
    width = w_all.shape[2]
    tile = 512
    rows = pl.BlockSpec((tile, d_model), lambda i: (i, 0))
    return pl.pallas_call(
        shared_kernel,
        out_shape=jax.ShapeDtypeStruct((tok_count, d_model), F32),
        grid=(tok_count // tile,),
        in_specs=[rows, pl.BlockSpec((3, d_model, width), lambda i: (0, 0, 0))],
        out_specs=rows,
        compiler_params=params(("arbitrary",)),
        cost_estimate=cost(6 * tok_count * d_model * width, 6 * tok_count * d_model),
        name="shared_part",
    )(x_blk, w_all)


def combine_kernel(n_base, where_of, halves, capacity, group, *refs):
    cnt_ref, tok_ref, gate_ref = refs[:3]
    bases = refs[3:3 + n_base]
    n_chunks = max(w[0] for w in where_of) + 1
    outs = refs[3 + n_base:3 + n_base + n_chunks]
    n_out = 2 if halves else 1
    pos = 3 + n_base + n_chunks
    y_refs = refs[pos:pos + n_out]
    acc, tmps, rows, wide, sem_in, sem_rows, sem_out = refs[pos + n_out:]
    tok_count, d_model = bases[0].shape
    n_col = d_model // LANES
    step = 256
    n_step = tok_count // step

    def in_copy(k, b):
        at = pl.ds(b * step, step)
        return pltpu.make_async_copy(bases[k].at[at], tmps.at[k, at], sem_in.at[k, b])

    def out_copy(b):
        at = b * step
        per_out = tok_count // n_out
        dst = y_refs[at // per_out].at[pl.ds(at % per_out, step)]
        return pltpu.make_async_copy(tmps.at[0, pl.ds(at, step)], dst, sem_out.at[b])

    def row_copy(i):
        c, local, slot, _ = where_of[i]
        return pltpu.make_async_copy(outs[c].at[local, slot], rows.at[i % 2], sem_rows.at[i % 2])

    for b in range(n_step):
        for k in range(n_base):
            in_copy(k, b).start()
    row_copy(0).start()

    for b in range(n_step):
        for k in range(n_base):
            in_copy(k, b).wait()

        @pl.loop(0, step // 32)
        def _(q):
            at = pl.multiple_of(b * step + q * 32, 32)
            val = tmps[0, pl.ds(at, 32), :]
            for k in range(1, n_base):
                val = val + tmps[k, pl.ds(at, 32), :]
            for j in range(n_col):
                acc[pl.ds(at * TILE + j, 32, stride=TILE), :] = val[:, j * LANES:(j + 1) * LANES]

    for i in range(len(where_of)):
        row_copy(i).wait()
        if i + 1 < len(where_of):
            row_copy(i + 1).start()
        e = where_of[i][3]
        slot = i % 2

        @pl.loop(0, capacity // 32)
        def _(q):
            at = pl.multiple_of(q * 32, 32)
            val = rows[slot, pl.ds(at, 32), :].astype(F32)
            for j in range(n_col):
                wide[pl.ds(at * TILE + j, 32, stride=TILE), :] = val[:, j * LANES:(j + 1) * LANES]

        @pl.loop(0, (cnt_ref[0, e] + (group - 1)) // group)
        def _(q):
            sums, toks = [], []
            for i in range(group):
                s = q * group + i
                t = tok_ref[0, e * capacity + s]
                g = gate_ref[0, e * tok_count + t]
                t = pl.multiple_of(t * TILE, TILE)
                toks.append(t)
                sums.append(acc[pl.ds(t, TILE), :] + g * wide[pl.ds(pl.multiple_of(s * TILE, TILE), TILE), :])
            for i in range(group):
                acc[pl.ds(toks[i], TILE), :] = sums[i]

    for b in range(n_step):

        @pl.loop(0, step // 32)
        def _(q):
            at = pl.multiple_of(b * step + q * 32, 32)
            for j in range(n_col):
                tmps[0, pl.ds(at, 32), j * LANES:(j + 1) * LANES] = acc[pl.ds(at * TILE + j, 32, stride=TILE), :]

        out_copy(b).start()
    for b in range(n_step):
        out_copy(b).wait()


def combine(cnt, toks, gates, bases, outs, slots, first, halves):
    tok_count, d_model = bases[0].shape
    capacity = outs[0].shape[2]
    where_of = []
    for c, o in enumerate(outs):
        for i in range(o.shape[0]):
            where_of.append((c, i, slots[c], first + len(where_of)))
    smem = pl.BlockSpec(memory_space=pltpu.SMEM)
    hbm = pl.BlockSpec(memory_space=pl.ANY)
    n_base = len(bases)
    if halves:
        out_shape = [jax.ShapeDtypeStruct((tok_count // 2, d_model), F32)] * 2
        out_specs = [hbm, hbm]
    else:
        out_shape, out_specs = jax.ShapeDtypeStruct((tok_count, d_model), F32), hbm
    return pl.pallas_call(
        functools.partial(combine_kernel, n_base, tuple(where_of), halves, capacity, 8),
        out_shape=out_shape,
        in_specs=[smem, smem, smem] + [hbm] * (n_base + len(outs)),
        out_specs=out_specs,
        scratch_shapes=[
            pltpu.VMEM(((tok_count + 1) * TILE, LANES), F32),
            pltpu.VMEM((n_base, tok_count, d_model), F32),
            pltpu.VMEM((2, capacity, d_model), BF16),
            pltpu.VMEM((capacity * TILE, LANES), F32),
            pltpu.SemaphoreType.DMA((n_base, tok_count // 256)),
            pltpu.SemaphoreType.DMA((2,)),
            pltpu.SemaphoreType.DMA((tok_count // 256,)),
        ],
        compiler_params=pltpu.CompilerParams(vmem_limit_bytes=VMEM_LIMIT),
        cost_estimate=cost(len(where_of) * capacity * tok_count * d_model, tok_count * d_model * 8),
        name="combine",
    )(cnt, toks, gates, *bases, *outs)


def assemble_kernel(me_ref, *refs):
    out_ref = refs[-1]
    for r, part in enumerate(refs[:-1]):
        rows = part.shape[1]
        at = pl.multiple_of((me_ref[0] ^ r) * rows, 16)
        for k in range(part.shape[0]):
            out_ref[k, pl.ds(at, rows), :] = part[k]


def assemble(me_arr, parts):
    n_arr, rows, width = parts[0].shape
    vmem = pl.BlockSpec(memory_space=pltpu.VMEM)
    return pl.pallas_call(
        assemble_kernel,
        out_shape=jax.ShapeDtypeStruct((n_arr, len(parts) * rows, width), BF16),
        in_specs=[pl.BlockSpec(memory_space=pltpu.SMEM)] + [vmem] * len(parts),
        out_specs=vmem,
        compiler_params=pltpu.CompilerParams(vmem_limit_bytes=VMEM_LIMIT),
        name="assemble",
    )(me_arr, *parts)


def finish_kernel(n_half, a_ref, b_ref, c_ref, d_ref, out_ref):
    @pl.when(pl.program_id(0) < n_half)
    def _():
        out_ref[...] = (a_ref[...] + b_ref[...]).astype(BF16)

    @pl.when(pl.program_id(0) >= n_half)
    def _():
        out_ref[...] = (c_ref[...] + d_ref[...]).astype(BF16)


def finish(top_sum, top_late, bot_sum, bot_late):
    rows, d_model = top_sum.shape
    tile = 256
    n_half = rows // tile
    top = pl.BlockSpec((tile, d_model), lambda i: (jnp.minimum(i, n_half - 1), 0))
    bot = pl.BlockSpec((tile, d_model), lambda i: (jnp.maximum(i - n_half, 0), 0))
    return pl.pallas_call(
        functools.partial(finish_kernel, n_half),
        out_shape=jax.ShapeDtypeStruct((2 * rows, d_model), BF16),
        grid=(2 * n_half,),
        in_specs=[top, top, bot, bot],
        out_specs=pl.BlockSpec((tile, d_model), lambda i: (i, 0)),
        compiler_params=params(("arbitrary",)),
        name="finish",
    )(top_sum, top_late, bot_sum, bot_late)


def solution(mesh):
    exp_n = mesh.shape["expert"]
    data_n = mesh.shape["data"]
    assert exp_n == 4 and data_n == 2
    tok_spec = P(("rep", "expert", "data"), None)
    group_axes = ("expert", "data")
    n_dev = exp_n * data_n

    def over_y(v):
        return lax.ppermute(v, "data", [(i, i ^ 1) for i in range(data_n)])

    def over_core(v):
        return lax.ppermute(v, "expert", [(i, i ^ 1) for i in range(exp_n)])

    def over_x(v):
        return lax.ppermute(v, "expert", [(i, i ^ 2) for i in range(exp_n)])

    def over_all(v, r):
        flip = (r & 1) * exp_n + (r >> 1)
        return lax.ppermute(v, ("data", "expert"), [(i, i ^ flip) for i in range(n_dev)])

    def device_fn(x_loc, idx_loc, gate_loc, wg_loc, wu_loc, wd_loc, wsg_loc, wsu_loc, wsd_loc):
        tok_count, _ = x_loc.shape
        top = idx_loc.shape[1]
        n_local, _, _ = wg_loc.shape
        n_mine = n_local // data_n
        capacity = capacity_of(tok_count, top, n_local * exp_n)
        y = lax.axis_index("data")
        p = lax.axis_index("expert")
        wdt_loc = jnp.swapaxes(wd_loc, 1, 2)

        meta = jnp.concatenate([idx_loc.T.astype(F32), gate_loc.T], axis=0)
        meta_rel = [meta]
        for r in range(1, n_dev):
            meta_rel.append(over_all(meta, r))

        blocks = [None] * n_dev
        blocks[0] = x_loc
        blocks[1] = over_y(x_loc)
        blocks[4] = over_x(x_loc)
        blocks[2] = over_core(x_loc)
        blocks[6] = over_core(blocks[4])
        blocks[3] = over_core(blocks[1])
        blocks[5] = over_x(blocks[1])
        blocks[7] = over_core(blocks[5])

        ws = jnp.stack([wsg_loc, wsu_loc, wsd_loc.T])
        rows_s, width_s = ws.shape[1], ws.shape[2] // n_dev
        ws = ws.reshape(3, rows_s, n_dev, width_s).transpose(2, 0, 1, 3)
        by_rel = (p * data_n + y) ^ jnp.arange(n_dev, dtype=jnp.int32)
        ws = jnp.take(ws, by_rel, axis=0)
        ws_parts = [ws[0]]
        for r in range(1, n_dev):
            ws_parts.append(over_all(ws[r], r))

        recvs = []
        start = 0
        for n in CHUNKS:
            at = (1 - y) * n_mine + start
            piece = jnp.stack([lax.dynamic_slice_in_dim(w, at, n, 0) for w in (wg_loc, wu_loc, wdt_loc)])
            recvs.append(over_y(piece))
            start += n

        meta_rel = jnp.stack(meta_rel)
        ids = meta_rel[:, :top].astype(jnp.int32)
        gts = meta_rel[:, top:]
        mine = p * n_local + y * n_mine + jnp.arange(n_mine, dtype=jnp.int32)
        hit = ids[:, None] == mine[None, :, None, None]
        chosen = jnp.any(hit, axis=2).reshape(n_dev * n_mine, tok_count)
        t_ids = jnp.arange(tok_count, dtype=jnp.int32)
        before = (t_ids[:, None] < t_ids[None, :]).astype(BF16)
        rank = jnp.dot(chosen.astype(BF16), before, preferred_element_type=F32).astype(jnp.int32)
        pos = jnp.where(chosen & (rank < capacity), rank, -1)
        pos_pad = jnp.pad(pos.reshape(n_dev, n_mine, tok_count), ((0, 0), (0, TILE), (0, 0)), constant_values=-1)

        last = [pos_pad]

        def after(*vals):
            done, vals = lax.optimization_barrier((last[0], vals))
            last[0] = done
            return vals if len(vals) > 1 else vals[0]

        xg = None

        def gather(r):
            nonlocal xg
            x_blk = after(blocks[r])
            xg = gather_rows(SLOT[r], n_dev, pos_pad[r], x_blk, xg, capacity)
            last[0] = xg

        base = [None] * n_dev
        shared_w = []

        def shared(r):
            if not shared_w:
                whole = assemble(by_rel[:1], after(*ws_parts))
                last[0] = whole
                shared_w.append(whole)
            x_blk = after(blocks[r])
            base[r] = shared_part(x_blk, *shared_w)
            last[0] = base[r]

        y_arr = y.astype(jnp.int32).reshape(1)

        def experts(c, slots=(0, n_dev)):
            start = sum(CHUNKS[:c])
            recv = after(recvs[c])
            out = expert_rows(start, CHUNKS[c], slots, y_arr, xg, wg_loc, wu_loc, wdt_loc, recv)
            last[0] = out
            return out

        lists = []

        def make_lists():
            p_in, ids_in, gts_in = after(pos, ids, gts)
            hit_in = ids_in[:, None] == mine[None, :, None, None]
            gate_of = jnp.sum(jnp.where(hit_in, gts_in[:, None], 0.0), axis=2).reshape(n_dev, 1, n_mine * tok_count)
            gate_of = jnp.pad(gate_of, ((0, 0), (0, 0), (0, LANES)))
            same = p_in[:, None, :] == jnp.arange(capacity, dtype=jnp.int32)[None, :, None]
            toks = jnp.sum(jnp.where(same, t_ids[None, None, :] - tok_count, 0), axis=2) + tok_count
            count = jnp.sum((p_in >= 0).astype(jnp.int32), axis=1).reshape(n_dev, 1, n_mine)
            toks = toks.reshape(n_dev, 1, n_mine * capacity)
            lists.extend([count, toks, gate_of])
            last[0] = (toks, gate_of)

        def part(r, bases, arrays, first, halves):
            count, toks, gate_of = lists
            outs_r = [o for o, _ in arrays]
            slots_r = [SLOT[r] - s0 for _, s0 in arrays]
            (b0, *rest) = bases
            args = [after(b0), *rest]
            out = combine(count[r], toks[r], gate_of[r], args, outs_r, slots_r, first, halves)
            last[0] = out[0] if halves else out
            return out

        gather(0)
        gather(2)
        gather(1)
        gather(4)
        gather(3)
        gather(6)
        make_lists()
        gather(5)
        gather(7)
        early = [(experts(0), 0)]
        shared(7)
        early.append((experts(1), 0))
        shared(5)
        shared(3)
        shared(1)
        early.append((experts(2), 0))
        shared(6)
        shared(4)
        early.append((experts(3), 0))
        diag_rows = early + [(experts(4, (0, 2)), 0)]
        mate7 = over_core(part(7, [base[7]], diag_rows, 0, False))
        full = early + [(experts(4, (2, n_dev)), 2)]
        diag = part(5, [base[5], mate7], diag_rows, 0, True)
        diag_x = over_x(diag[0])
        diag_y = over_y(diag[1])
        mate6 = over_core(part(6, [base[6]], full, 0, False))
        mate3 = over_core(part(3, [base[3]], full, 0, False))
        to_x = part(4, [base[4], mate6], full, 0, True)
        x_top = over_x(to_x[0])
        to_y = part(1, [base[1], mate3], full, 0, True)
        y_bot = over_y(to_y[1])
        shared(2)
        up_x, up_y, to_x1, to_y0 = after(diag_y, diag_x, to_x[1], to_y[0])
        last_x, last_y = to_x1 + up_x, to_y0 + up_y
        last[0] = (last_x, last_y)
        x_bot = over_x(last_x)
        y_top = over_y(last_y)
        mate2 = over_core(part(2, [base[2]], full, 0, False))
        shared(0)
        own = part(0, [base[0], mate2], full, 0, True)
        h = tok_count // 2
        sum_top = x_loc[:h].astype(F32) + own[0] + x_top
        sum_bot = x_loc[h:].astype(F32) + own[1] + y_bot
        sum_top, sum_bot = lax.optimization_barrier((sum_top, sum_bot))
        return finish(sum_top, y_top, sum_bot, x_bot)

    in_specs = (tok_spec, tok_spec, tok_spec, P("expert", "data", None), P("expert", "data", None), P("expert", None, "data"), P(group_axes, None), P(group_axes, None), P(None, group_axes))
    return jax.shard_map(device_fn, mesh=mesh, in_specs=in_specs, out_specs=tok_spec, check_vma=False)
```
